8 devices in a mesh: dp: 2 (over y, z), tp: 4 (over x, core).
Axes of the slice: x: 2, y: 2, z: 1, core: 2. Of those that a mesh axis runs over, the one named last changes fastest.
Arguments:
- x: bfloat16 [128, 3072], P('dp'), parts along dimension 0
- k_cache: bfloat16 [128, 1024, 32, 96], P('dp', None, 'tp'), parts along dimension 0
- v_cache: bfloat16 [128, 1024, 32, 96], P('dp', None, 'tp'), parts along dimension 0
- gain_a: bfloat16 [3072], replicated
- wq: bfloat16 [3072, 3072], P(None, 'tp')
- wo: bfloat16 [3072, 3072], P('tp')
- gain_m: bfloat16 [3072], replicated
- w_gate: bfloat16 [3072, 8192], P(None, 'tp')
- w_up: bfloat16 [3072, 8192], P(None, 'tp')
- w_down: bfloat16 [8192, 3072], P('tp')
Outputs:
- output: bfloat16 [128, 3072], P('dp'), parts along dimension 0
There are 2 independent parts. The reference program is written for one: setup_inputs(seed, part) draws one part's arguments, and reference() takes and returns one part's arrays. A program takes and returns all parts, laid end to end along the dimension named above; an argument that names none is the same for every part.
All inputs are finite; a program needn't handle non-finite values.
Results may differ from the reference program's by a relative error of at most 0.017.
Values are sent between devices in bfloat16 or wider.
A program may use at most 2 GiB of HBM per device.

```python
import jax
import jax.numpy as jnp
from jax import lax

BATCH = 64
CACHE = 1024
D = 3072
HEADS = 32
KV_HEADS = 32
HEAD = 96
FF = 8192
THETA = 10000


def setup_inputs(seed: int = 0, part: int = 0) -> dict:
    kx, kc, kw, kn, kq, ko, km, kg, ku, kd = jax.random.split(jax.random.key(seed), 10)
    kx, kc, kw = (jax.random.fold_in(k, part) for k in (kx, kc, kw))

    def weights(key, rows, columns):
        return jax.random.normal(key, (rows, columns), jnp.float32) * rows**-0.5

    drawn = {
        "x": jax.random.normal(kx, (BATCH, D), jnp.float32),
        "k_cache": 2 * jax.random.normal(kc, (BATCH, CACHE, KV_HEADS, HEAD), jnp.float32),
        "v_cache": 4 * jax.random.normal(kw, (BATCH, CACHE, KV_HEADS, HEAD), jnp.float32),
        "gain_a": 1 + 0.1 * jax.random.normal(kn, (D,), jnp.float32),
        "wq": 2 * weights(kq, D, HEADS * HEAD),
        "wo": weights(ko, HEADS * HEAD, D),
        "gain_m": 1 + 0.1 * jax.random.normal(km, (D,), jnp.float32),
        "w_gate": weights(kg, D, FF),
        "w_up": weights(ku, D, FF),
        "w_down": 2 * weights(kd, FF, D),
    }
    return {k: v.astype(jnp.bfloat16) for k, v in drawn.items()}


def normed(x, gain):
    wide = x.astype(jnp.float32)
    scale = lax.rsqrt(jnp.mean(wide * wide, -1, keepdims=True) + 1e-6)
    return (wide * scale * gain.astype(jnp.float32)).astype(jnp.bfloat16)


def turned(t, place, theta):
    half = t.shape[-1] // 2
    angle = place.astype(jnp.float32)[:, None] * theta ** (-jnp.arange(half, dtype=jnp.float32) / half)
    cos, sin = jnp.cos(angle)[:, None], jnp.sin(angle)[:, None]
    a, b = t[..., :half].astype(jnp.float32), t[..., half:].astype(jnp.float32)
    return jnp.concatenate([a * cos - b * sin, b * cos + a * sin], -1).astype(jnp.bfloat16)


def matmul(a, w):
    return jnp.dot(a, w, preferred_element_type=jnp.float32).astype(jnp.bfloat16)


def einsum(form, a, b):
    return jnp.einsum(form, a.astype(jnp.float32), b.astype(jnp.float32))


def seen_by(a, wq, k_cache, v_cache, head, theta):
    batch, cache, kv_heads = k_cache.shape[:3]
    place = jnp.full((batch,), cache - 1)
    q = turned(matmul(a, wq).reshape(batch, -1, head), place, theta).reshape(batch, kv_heads, -1, head)
    scores = einsum("bgsd,bugd->bgsu", q, k_cache) * head**-0.5
    weights = jax.nn.softmax(scores, -1).astype(jnp.bfloat16)
    return einsum("bgsu,bugd->bgsd", weights, v_cache).astype(jnp.bfloat16).reshape(batch, -1)


def hidden_of(b, w_gate, w_up):
    gate = jnp.dot(b, w_gate, preferred_element_type=jnp.float32)
    up = jnp.dot(b, w_up, preferred_element_type=jnp.float32)
    return (jax.nn.silu(gate) * up).astype(jnp.bfloat16)


def reference(x, k_cache, v_cache, gain_a, wq, wo, gain_m, w_gate, w_up, w_down):
    seen = seen_by(normed(x, gain_a), wq, k_cache, v_cache, HEAD, THETA)
    h = (x.astype(jnp.float32) + jnp.dot(seen, wo, preferred_element_type=jnp.float32)).astype(jnp.bfloat16)
    hidden = hidden_of(normed(h, gain_m), w_gate, w_up)
    return (h.astype(jnp.float32) + jnp.dot(hidden, w_down, preferred_element_type=jnp.float32)).astype(jnp.bfloat16)
```

```python
import jax
import jax.numpy as jnp
import numpy as np
from jax import lax
from jax.experimental import pallas as pl
from jax.experimental.pallas import tpu as pltpu
from jax.sharding import PartitionSpec as P

HEAD = 96
THETA = 10000
EPS = 1e-6
SEQS = 2
SLOTS = 3
GROUP = 16
FCHUNK = 512
DCHUNK = 512

F32, BF16 = jnp.float32, jnp.bfloat16
NT = (((1,), (1,)), ((), ()))


def rotary_table(heads, head, place):
    half = head // 2
    angle = np.float32(place) * np.float32(THETA) ** (-np.arange(half, dtype=np.float32) / np.float32(half))
    cos, sin, zero = np.cos(angle), np.sin(angle), np.zeros(half, np.float32)
    rows = [np.concatenate(r) for r in ((cos, cos), (-sin, zero), (zero, sin))]
    return np.stack([np.tile(r, heads) for r in rows]).astype(np.float32)


def dot(a, b):
    return jnp.dot(a, b, preferred_element_type=F32)


def normed(wide, gain):
    scale = lax.rsqrt(jnp.mean(wide * wide, -1, keepdims=True) + EPS)
    return (wide * scale * gain).astype(BF16)


def layer_kernel(
    x_hbm, k_hbm, v_hbm, ga_hbm, wq_hbm, wo_hbm, gm_hbm, wg_hbm, wu_hbm, wd_hbm, trig_hbm,
    y_ref,
    k_buf, v_buf, wg, wu, wd, wo, x, ga, gm, trig,
    q, o, term, send1, recv1, send2, recv2, h, hid,
    send3, recv3, send4, recv4,
    ksem, vsem, wsem, gsem, usem, dsem, isem,
    s1, r1, s2, r2, s3, r3, s4, r4, s5, r5, s6, r6,
):
    rows, d = x.shape
    width = q.shape[1]
    ff = hid.shape[1]
    half = d // 2
    heads = width // HEAD
    t = lax.axis_index("tp")
    core = lax.rem(t, 2)
    other = 1 - core
    partner = t + 1 - 2 * core
    across = lax.rem(t + 2, 4)
    blocks = rows // SEQS
    per_group = GROUP // SEQS
    groups = rows // GROUP
    nf, nd = ff // FCHUNK, d // DCHUNK
    dh = DCHUNK // 2

    barrier = pltpu.get_barrier_semaphore()
    for peer in (partner, across):
        pl.semaphore_signal(barrier, inc=1, device_id={"tp": peer}, device_id_type=pl.DeviceIdType.MESH)

    def cache_copies(b, slot):
        at = pl.ds(b * SEQS, SEQS)
        return (
            pltpu.make_async_copy(k_hbm.at[at], k_buf.at[slot], ksem.at[slot]),
            pltpu.make_async_copy(v_hbm.at[at], v_buf.at[slot], vsem.at[slot]),
        )

    wq = wg.at[:, pl.ds(0, width)]
    first = [
        pltpu.make_async_copy(x_hbm, x, isem.at[0]),
        pltpu.make_async_copy(ga_hbm, ga, isem.at[1]),
        pltpu.make_async_copy(trig_hbm, trig, isem.at[2]),
        pltpu.make_async_copy(wq_hbm, wq, isem.at[3]),
    ]
    later = [
        pltpu.make_async_copy(gm_hbm, gm, isem.at[4]),
        pltpu.make_async_copy(wo_hbm, wo, wsem),
    ]
    gate_copy = [
        pltpu.make_async_copy(wg_hbm.at[:, pl.ds(c * FCHUNK, FCHUNK)], wg.at[:, pl.ds(c * FCHUNK, FCHUNK)], gsem.at[c])
        for c in range(nf)
    ]
    up_copy = [
        pltpu.make_async_copy(wu_hbm.at[:, pl.ds(c * FCHUNK, FCHUNK)], wu.at[:, pl.ds(c * FCHUNK, FCHUNK)], usem.at[c])
        for c in range(nf)
    ]
    down_copy = [
        pltpu.make_async_copy(wd_hbm.at[:, pl.ds(c * DCHUNK, DCHUNK)], wd.at[:, pl.ds(c * DCHUNK, DCHUNK)], dsem.at[c])
        for c in range(nd)
    ]

    for c in first:
        c.start()
    for s in range(SLOTS):
        for c in cache_copies(s, s):
            c.start()
    for c in later:
        c.start()

    for c in first[:3]:
        c.wait()
    a = normed(x[...].astype(F32), ga[...].astype(F32))
    first[3].wait()
    q0 = dot(a, wq[...]).astype(BF16).astype(F32)
    ahead = pltpu.roll(q0, width - HEAD // 2, 1)
    behind = pltpu.roll(q0, HEAD // 2, 1)
    q[...] = (q0 * trig[0:1, :] + ahead * trig[1:2, :] + behind * trig[2:3, :]).astype(BF16).astype(F32)

    lane = lax.broadcasted_iota(jnp.int32, (heads, width), 1)
    top = lax.broadcasted_iota(jnp.int32, (heads, width), 0) * HEAD
    own_head = (lane >= top) & (lane < top + HEAD)

    pl.semaphore_wait(barrier, 2)

    def to(peer, src, dst, ssem, rsem):
        return pltpu.make_async_remote_copy(
            src_ref=src, dst_ref=dst, send_sem=ssem, recv_sem=rsem,
            device_id={"tp": peer}, device_id_type=pl.DeviceIdType.MESH,
        )

    mine = pl.ds(pl.multiple_of(core * half, half), half)
    theirs = pl.ds(pl.multiple_of(other * half, half), half)

    def rows_of(g):
        return pl.ds(pl.multiple_of(g * GROUP, GROUP), GROUP)

    def copy1(g):
        return to(partner, send1.at[rows_of(g)], recv1.at[rows_of(g)], s1.at[g], r1.at[g])

    def copy2(g):
        return to(across, send2.at[rows_of(g)], recv2.at[rows_of(g)], s2.at[g], r2.at[g])

    def copy3(g):
        return to(partner, h.at[rows_of(g), mine], h.at[rows_of(g), mine], s3.at[g], r3.at[g])

    def project(g):
        at = rows_of(g)
        seen = o[at, :].astype(BF16)
        send1[at, :] = dot(seen, wo[:, theirs]).astype(BF16)
        copy1(g).start()
        term[at, :] = dot(seen, wo[:, mine])

    def pair_sum(g):
        at = rows_of(g)
        copy1(g).wait_recv()
        send2[at, :] = (term[at, :] + recv1[at, :].astype(F32)).astype(BF16)
        copy2(g).start()

    def finish(g):
        at = rows_of(g)
        copy2(g).wait_recv()
        total = send2[at, :].astype(F32) + recv2[at, :].astype(F32)
        h[at, mine] = (x[at, mine].astype(F32) + total).astype(BF16)
        copy3(g).start()

    def softmax(scores):
        scores = scores * HEAD**-0.5
        e = jnp.exp(scores - jnp.max(scores, -1, keepdims=True))
        return (e / jnp.sum(e, -1, keepdims=True)).astype(BF16)

    later[1].wait()

    def block(b, carry):
        slot = lax.rem(b, SLOTS)
        kc, vc = cache_copies(b, slot)
        kc.wait()
        vc.wait()
        scores = []
        for i in range(SEQS):
            row = q[pl.ds(b * SEQS + i, 1), :]
            spread = jnp.where(own_head, jnp.broadcast_to(row, (heads, width)), 0.0).astype(BF16)
            scores.append(dot(spread, k_buf[slot, i]))
        for i in range(SEQS):
            weights = softmax(scores[i])
            out = lax.dot_general(weights, v_buf[slot, i], NT, preferred_element_type=F32)
            o[pl.ds(b * SEQS + i, 1), :] = jnp.sum(jnp.where(own_head, out, 0.0), 0, keepdims=True)

        @pl.when(b + SLOTS < blocks)
        def _():
            for c in cache_copies(b + SLOTS, slot):
                c.start()

        for n in range(SLOTS):
            @pl.when(b == blocks - SLOTS + n)
            def _():
                gate_copy[n].start()
                up_copy[n].start()

        g = lax.div(b, per_group)
        step = lax.rem(b, per_group)

        @pl.when(step == per_group - 1)
        def _():
            project(g)

        @pl.when((step == 0) & (b > 0))
        def _():
            pair_sum(g - 1)

        @pl.when((step == 3) & (b > per_group))
        def _():
            finish(g - 1)

        return carry

    lax.fori_loop(0, blocks, block, 0)
    for n in range(SLOTS, nf):
        gate_copy[n].start()
        up_copy[n].start()
    for c in down_copy:
        c.start()

    pair_sum(groups - 1)
    finish(groups - 1)
    later[0].wait()
    for g in range(groups):
        copy3(g).wait_recv()
    b_states = normed(h[...].astype(F32), gm[...].astype(F32))

    for n in range(nf):
        at = pl.ds(n * FCHUNK, FCHUNK)
        gate_copy[n].wait()
        gate = dot(b_states, wg[:, at])
        up_copy[n].wait()
        up = dot(b_states, wu[:, at])
        hid[:, at] = (gate * jax.nn.sigmoid(gate) * up).astype(BF16)

    def columns(n, which):
        return pl.ds(pl.multiple_of(n * DCHUNK + which * dh, dh), dh)

    def part(n):
        return pl.ds(n * dh, dh)

    def copy4(n):
        return to(partner, send3.at[:, part(n)], recv3.at[:, part(n)], s4.at[n], r4.at[n])

    def copy5(n):
        return to(across, send4.at[:, part(n)], recv4.at[:, part(n)], s5.at[n], r5.at[n])

    def copy6(n):
        return to(partner, y_ref.at[:, columns(n, core)], y_ref.at[:, columns(n, core)], s6.at[n], r6.at[n])

    term2 = term
    def down(n):
        down_copy[n].wait()
        send3[:, part(n)] = dot(hid[...], wd[:, columns(n, other)]).astype(BF16)
        copy4(n).start()
        term2[:, part(n)] = dot(hid[...], wd[:, columns(n, core)])

    def down_pair(n):
        copy4(n).wait_recv()
        send4[:, part(n)] = (term2[:, part(n)] + recv3[:, part(n)].astype(F32)).astype(BF16)
        copy5(n).start()

    def down_finish(n):
        copy5(n).wait_recv()
        total = send4[:, part(n)].astype(F32) + recv4[:, part(n)].astype(F32)
        y_ref[:, columns(n, core)] = (h[:, columns(n, core)].astype(F32) + total).astype(BF16)
        copy6(n).start()

    lag = 3
    for n in range(nd + lag):
        if n < nd:
            down(n)
        if n >= lag:
            down_pair(n - lag)
    for n in range(nd):
        down_finish(n)
    for g in range(groups):
        copy1(g).wait_send()
        copy2(g).wait_send()
        copy3(g).wait_send()
    for n in range(nd):
        copy4(n).wait_send()
        copy5(n).wait_send()
        copy6(n).wait()


def solution(mesh):
    def step(x, k_cache, v_cache, gain_a, wq, wo, gain_m, w_gate, w_up, w_down):
        rows, d = x.shape
        cache, heads = k_cache.shape[1:3]
        width = heads * HEAD
        ff = w_gate.shape[1]
        turned_cache = [c.transpose(0, 2, 3, 1).reshape(rows, width, cache) for c in (k_cache, v_cache)]
        trig = jnp.asarray(rotary_table(heads, HEAD, cache - 1))
        gains = [g.reshape(1, d) for g in (gain_a, gain_m)]
        half, groups, nf, nd = d // 2, rows // GROUP, ff // FCHUNK, d // DCHUNK
        dma = pltpu.SemaphoreType.DMA
        return pl.pallas_call(
            layer_kernel,
            out_shape=jax.ShapeDtypeStruct((rows, d), BF16),
            in_specs=[pl.BlockSpec(memory_space=pl.ANY)] * 11,
            out_specs=pl.BlockSpec(memory_space=pltpu.VMEM),
            scratch_shapes=[
                pltpu.VMEM((SLOTS, SEQS, width, cache), BF16),
                pltpu.VMEM((SLOTS, SEQS, width, cache), BF16),
                pltpu.VMEM((d, ff), BF16),
                pltpu.VMEM((d, ff), BF16),
                pltpu.VMEM((ff, d), BF16),
                pltpu.VMEM((width, d), BF16),
                pltpu.VMEM((rows, d), BF16),
                pltpu.VMEM((1, d), BF16),
                pltpu.VMEM((1, d), BF16),
                pltpu.VMEM((3, width), F32),
                pltpu.VMEM((rows, width), F32),
                pltpu.VMEM((rows, width), F32),
                pltpu.VMEM((rows, half), F32),
                pltpu.VMEM((rows, half), BF16),
                pltpu.VMEM((rows, half), BF16),
                pltpu.VMEM((rows, half), BF16),
                pltpu.VMEM((rows, half), BF16),
                pltpu.VMEM((rows, d), BF16),
                pltpu.VMEM((rows, ff), BF16),
                pltpu.VMEM((rows, half), BF16),
                pltpu.VMEM((rows, half), BF16),
                pltpu.VMEM((rows, half), BF16),
                pltpu.VMEM((rows, half), BF16),
                dma((SLOTS,)), dma((SLOTS,)), dma, dma((nf,)), dma((nf,)), dma((nd,)), dma((5,)),
                *[dma((groups,)) for _ in range(6)],
                *[dma((nd,)) for _ in range(6)],
            ],
            compiler_params=pltpu.CompilerParams(
                collective_id=0, has_side_effects=True, vmem_limit_bytes=67043328
            ),
            name="decode_layer",
        )(x, *turned_cache, gains[0], wq, wo, gains[1], w_gate, w_up, w_down, trig)

    states, cache, columns, rows_of = P("dp", None), P("dp", None, "tp", None), P(None, "tp"), P("tp", None)
    return jax.shard_map(
        step,
        mesh=mesh,
        in_specs=(states, cache, cache, P(None), columns, rows_of, P(None), columns, columns, rows_of),
        out_specs=states,
        check_vma=False,
    )
```

```python
import jax
import jax.numpy as jnp
import numpy as np
from jax import lax
from jax.experimental import pallas as pl
from jax.experimental.pallas import tpu as pltpu
from jax.sharding import PartitionSpec as P

HEAD = 96
THETA = 10000
EPS = 1e-6
SEQS = 2
SLOTS = 3
GROUP = 16
FCHUNK = 512
DCHUNK = 512

F32, BF16 = jnp.float32, jnp.bfloat16
NT = (((1,), (1,)), ((), ()))


def rotary_table(heads, head, place):
    half = head // 2
    angle = np.float32(place) * np.float32(THETA) ** (-np.arange(half, dtype=np.float32) / np.float32(half))
    cos, sin, zero = np.cos(angle), np.sin(angle), np.zeros(half, np.float32)
    rows = [np.concatenate(r) for r in ((cos, cos), (-sin, zero), (zero, sin))]
    return np.stack([np.tile(r, heads) for r in rows]).astype(np.float32)


def dot(a, b):
    return jnp.dot(a, b, preferred_element_type=F32)


def normed(wide, gain):
    scale = lax.rsqrt(jnp.mean(wide * wide, -1, keepdims=True) + EPS)
    return (wide * scale * gain).astype(BF16)


def layer_kernel(
    x_hbm, k_hbm, v_hbm, ga_hbm, wq_hbm, wo_hbm, gm_hbm, wg_hbm, wu_hbm, wd_hbm, trig_hbm,
    y_ref,
    k_buf, v_buf, wg, wu, wd, wo, x, ga, gm, trig,
    q, o, term, send1, recv1, send2, recv2, h, hid,
    send3, recv3, send4, recv4,
    ksem, vsem, wsem, gsem, usem, dsem, isem,
    s1, r1, s2, r2, s3, r3, s4, r4, s5, r5, s6, r6,
):
    rows, d = x.shape
    width = q.shape[1]
    ff = hid.shape[1]
    half = d // 2
    heads = width // HEAD
    t = lax.axis_index("tp")
    core = lax.rem(t, 2)
    other = 1 - core
    partner = t + 1 - 2 * core
    across = lax.rem(t + 2, 4)
    blocks = rows // SEQS
    per_group = GROUP // SEQS
    groups = rows // GROUP
    nf, nd = ff // FCHUNK, d // DCHUNK
    dh = DCHUNK // 2

    barrier = pltpu.get_barrier_semaphore()
    for peer in (partner, across):
        pl.semaphore_signal(barrier, inc=1, device_id={"tp": peer}, device_id_type=pl.DeviceIdType.MESH)

    def cache_copies(b, slot):
        at = pl.ds(b * SEQS, SEQS)
        return (
            pltpu.make_async_copy(k_hbm.at[at], k_buf.at[slot], ksem.at[slot]),
            pltpu.make_async_copy(v_hbm.at[at], v_buf.at[slot], vsem.at[slot]),
        )

    wq = wg.at[:, pl.ds(0, width)]
    first = [
        pltpu.make_async_copy(x_hbm, x, isem.at[0]),
        pltpu.make_async_copy(ga_hbm, ga, isem.at[1]),
        pltpu.make_async_copy(trig_hbm, trig, isem.at[2]),
        pltpu.make_async_copy(wq_hbm, wq, isem.at[3]),
    ]
    later = [
        pltpu.make_async_copy(gm_hbm, gm, isem.at[4]),
        pltpu.make_async_copy(wo_hbm, wo, wsem),
    ]
    gate_copy = [
        pltpu.make_async_copy(wg_hbm.at[:, pl.ds(c * FCHUNK, FCHUNK)], wg.at[:, pl.ds(c * FCHUNK, FCHUNK)], gsem.at[c])
        for c in range(nf)
    ]
    up_copy = [
        pltpu.make_async_copy(wu_hbm.at[:, pl.ds(c * FCHUNK, FCHUNK)], wu.at[:, pl.ds(c * FCHUNK, FCHUNK)], usem.at[c])
        for c in range(nf)
    ]
    down_copy = [
        pltpu.make_async_copy(wd_hbm.at[:, pl.ds(c * DCHUNK, DCHUNK)], wd.at[:, pl.ds(c * DCHUNK, DCHUNK)], dsem.at[c])
        for c in range(nd)
    ]

    for c in first:
        c.start()
    for s in range(SLOTS):
        for c in cache_copies(s, s):
            c.start()
    for c in later:
        c.start()

    for c in first[:3]:
        c.wait()
    with jax.named_scope('norm_a'):
        a = normed(x[...].astype(F32), ga[...].astype(F32).reshape(1, d))
    first[3].wait()
    q0 = dot(a, wq[...]).astype(BF16).astype(F32)
    ahead = pltpu.roll(q0, width - HEAD // 2, 1)
    behind = pltpu.roll(q0, HEAD // 2, 1)
    q[...] = (q0 * trig[0:1, :] + ahead * trig[1:2, :] + behind * trig[2:3, :]).astype(BF16).astype(F32)

    lane = lax.broadcasted_iota(jnp.int32, (heads, width), 1)
    top = lax.broadcasted_iota(jnp.int32, (heads, width), 0) * HEAD
    own_head = (lane >= top) & (lane < top + HEAD)

    pl.semaphore_wait(barrier, 2)

    def to(peer, src, dst, ssem, rsem):
        return pltpu.make_async_remote_copy(
            src_ref=src, dst_ref=dst, send_sem=ssem, recv_sem=rsem,
            device_id={"tp": peer}, device_id_type=pl.DeviceIdType.MESH,
        )

    mine = pl.ds(pl.multiple_of(core * half, half), half)
    theirs = pl.ds(pl.multiple_of(other * half, half), half)

    def rows_of(g):
        return pl.ds(pl.multiple_of(g * GROUP, GROUP), GROUP)

    def copy1(g):
        return to(partner, send1.at[rows_of(g)], recv1.at[rows_of(g)], s1.at[g], r1.at[g])

    def copy2(g):
        return to(across, send2.at[rows_of(g)], recv2.at[rows_of(g)], s2.at[g], r2.at[g])

    def copy3(g):
        return to(partner, h.at[rows_of(g), mine], h.at[rows_of(g), mine], s3.at[g], r3.at[g])

    def project(g):
        at = rows_of(g)
        seen = o[at, :].astype(BF16)
        send1[at, :] = dot(seen, wo[:, theirs]).astype(BF16)
        copy1(g).start()
        term[at, :] = dot(seen, wo[:, mine])

    def pair_sum(g):
        at = rows_of(g)
        copy1(g).wait_recv()
        send2[at, :] = (term[at, :] + recv1[at, :].astype(F32)).astype(BF16)
        copy2(g).start()

    def finish(g):
        at = rows_of(g)
        copy2(g).wait_recv()
        total = send2[at, :].astype(F32) + recv2[at, :].astype(F32)
        h[at, mine] = (x[at, mine].astype(F32) + total).astype(BF16)
        copy3(g).start()

    def softmax(scores):
        scores = scores * HEAD**-0.5
        e = jnp.exp(scores - jnp.max(scores, -1, keepdims=True))
        return (e / jnp.sum(e, -1, keepdims=True)).astype(BF16)

    later[1].wait()

    def block(b, carry):
        slot = lax.rem(b, SLOTS)
        kc, vc = cache_copies(b, slot)
        with jax.named_scope('wait_cache'):
            kc.wait()
            vc.wait()
        scores = []
        for i in range(SEQS):
            row = q[pl.ds(b * SEQS + i, 1), :]
            spread = jnp.where(own_head, jnp.broadcast_to(row, (heads, width)), 0.0).astype(BF16)
            scores.append(dot(spread, k_buf[slot, i]))
        for i in range(SEQS):
            weights = softmax(scores[i])
            out = lax.dot_general(weights, v_buf[slot, i], NT, preferred_element_type=F32)
            o[pl.ds(b * SEQS + i, 1), :] = jnp.sum(jnp.where(own_head, out, 0.0), 0, keepdims=True)

        @pl.when(b + SLOTS < blocks)
        def _():
            for c in cache_copies(b + SLOTS, slot):
                c.start()

        for n in range(SLOTS):
            @pl.when(b == blocks - SLOTS + n)
            def _():
                gate_copy[n].start()
                up_copy[n].start()

        g = lax.div(b, per_group)
        step = lax.rem(b, per_group)

        @pl.when(step == per_group - 1)
        def _():
            with jax.named_scope('project'):
                project(g)

        @pl.when((step == 0) & (b > 0))
        def _():
            with jax.named_scope('pair_sum'):
                pair_sum(g - 1)

        @pl.when((step == 3) & (b > per_group))
        def _():
            with jax.named_scope('finish'):
                finish(g - 1)

        return carry

    lax.fori_loop(0, blocks, block, 0)
    for n in range(SLOTS, nf):
        gate_copy[n].start()
        up_copy[n].start()
    for c in down_copy:
        c.start()

    with jax.named_scope('pair_sum'):
        pair_sum(groups - 1)
    with jax.named_scope('finish'):
        finish(groups - 1)
    later[0].wait()
    with jax.named_scope('wait_h'):
        for g in range(groups):
            copy3(g).wait_recv()
    with jax.named_scope('norm_m'):
        b_states = normed(h[...].astype(F32), gm[...].astype(F32).reshape(1, d))

    for n in range(nf):
        at = pl.ds(n * FCHUNK, FCHUNK)
        with jax.named_scope('wait_gate'):
            gate_copy[n].wait()
        gate = dot(b_states, wg[:, at])
        with jax.named_scope('wait_up'):
            up_copy[n].wait()
        up = dot(b_states, wu[:, at])
        hid[:, at] = (gate * jax.nn.sigmoid(gate) * up).astype(BF16)

    def columns(n, which):
        return pl.ds(pl.multiple_of(n * DCHUNK + which * dh, dh), dh)

    def part(n):
        return pl.ds(n * dh, dh)

    def copy4(n):
        return to(partner, send3.at[:, part(n)], recv3.at[:, part(n)], s4.at[n], r4.at[n])

    def copy5(n):
        return to(across, send4.at[:, part(n)], recv4.at[:, part(n)], s5.at[n], r5.at[n])

    def copy6(n):
        return to(partner, y_ref.at[:, columns(n, core)], y_ref.at[:, columns(n, core)], s6.at[n], r6.at[n])

    term2 = term
    def down(n):
        down_copy[n].wait()
        send3[:, part(n)] = dot(hid[...], wd[:, columns(n, other)]).astype(BF16)
        copy4(n).start()
        term2[:, part(n)] = dot(hid[...], wd[:, columns(n, core)])

    def down_pair(n):
        copy4(n).wait_recv()
        send4[:, part(n)] = (term2[:, part(n)] + recv3[:, part(n)].astype(F32)).astype(BF16)
        copy5(n).start()

    def down_finish(n):
        copy5(n).wait_recv()
        total = send4[:, part(n)].astype(F32) + recv4[:, part(n)].astype(F32)
        y_ref[:, columns(n, core)] = (h[:, columns(n, core)].astype(F32) + total).astype(BF16)
        copy6(n).start()

    lag = 3
    for n in range(nd + lag):
        if n < nd:
            with jax.named_scope('down'):
                down(n)
        if n >= lag:
            with jax.named_scope('down_pair'):
                down_pair(n - lag)
    for n in range(nd):
        with jax.named_scope('down_finish'):
            down_finish(n)
    for g in range(groups):
        copy1(g).wait_send()
        copy2(g).wait_send()
        copy3(g).wait_send()
    for n in range(nd):
        copy4(n).wait_send()
        copy5(n).wait_send()
        copy6(n).wait()


def solution(mesh):
    def step(x, k_cache, v_cache, gain_a, wq, wo, gain_m, w_gate, w_up, w_down):
        rows, d = x.shape
        cache, heads = k_cache.shape[1:3]
        width = heads * HEAD
        ff = w_gate.shape[1]
        turned_cache = [c.transpose(0, 2, 3, 1).reshape(rows, width, cache) for c in (k_cache, v_cache)]
        trig = jnp.asarray(rotary_table(heads, HEAD, cache - 1))
        half, groups, nf, nd = d // 2, rows // GROUP, ff // FCHUNK, d // DCHUNK
        dma = pltpu.SemaphoreType.DMA
        return pl.pallas_call(
            layer_kernel,
            out_shape=jax.ShapeDtypeStruct((rows, d), BF16),
            in_specs=[pl.BlockSpec(memory_space=pl.ANY)] * 11,
            out_specs=pl.BlockSpec(memory_space=pltpu.VMEM),
            scratch_shapes=[
                pltpu.VMEM((SLOTS, SEQS, width, cache), BF16),
                pltpu.VMEM((SLOTS, SEQS, width, cache), BF16),
                pltpu.VMEM((d, ff), BF16),
                pltpu.VMEM((d, ff), BF16),
                pltpu.VMEM((ff, d), BF16),
                pltpu.VMEM((width, d), BF16),
                pltpu.VMEM((rows, d), BF16),
                pltpu.VMEM((d,), BF16),
                pltpu.VMEM((d,), BF16),
                pltpu.VMEM((3, width), F32),
                pltpu.VMEM((rows, width), F32),
                pltpu.VMEM((rows, width), F32),
                pltpu.VMEM((rows, half), F32),
                pltpu.VMEM((rows, half), BF16),
                pltpu.VMEM((rows, half), BF16),
                pltpu.VMEM((rows, half), BF16),
                pltpu.VMEM((rows, half), BF16),
                pltpu.VMEM((rows, d), BF16),
                pltpu.VMEM((rows, ff), BF16),
                pltpu.VMEM((rows, half), BF16),
                pltpu.VMEM((rows, half), BF16),
                pltpu.VMEM((rows, half), BF16),
                pltpu.VMEM((rows, half), BF16),
                dma((SLOTS,)), dma((SLOTS,)), dma, dma((nf,)), dma((nf,)), dma((nd,)), dma((5,)),
                *[dma((groups,)) for _ in range(6)],
                *[dma((nd,)) for _ in range(6)],
            ],
            compiler_params=pltpu.CompilerParams(
                collective_id=0, has_side_effects=True, vmem_limit_bytes=67043328
            ),
            name="decode_layer",
        )(x, *turned_cache, gain_a, wq, wo, gain_m, w_gate, w_up, w_down, trig)

    states, cache, columns, rows_of = P("dp", None), P("dp", None, "tp", None), P(None, "tp"), P("tp", None)
    return jax.shard_map(
        step,
        mesh=mesh,
        in_specs=(states, cache, cache, P(None), columns, rows_of, P(None), columns, columns, rows_of),
        out_specs=states,
        check_vma=False,
    )
```

```python
import jax
import jax.numpy as jnp
import numpy as np
from jax import lax
from jax.experimental import pallas as pl
from jax.experimental.pallas import tpu as pltpu
from jax.sharding import PartitionSpec as P

HEAD = 96
THETA = 10000
EPS = 1e-6
SEQS = 2
SLOTS = 3
GROUP = 16
QCHUNK = 768
FCHUNK = 512
DCHUNK = 512
LAG = 2

F32, BF16 = jnp.float32, jnp.bfloat16
NT = (((1,), (1,)), ((), ()))


def rotary_table(heads, head, place):
    half = head // 2
    angle = np.float32(place) * np.float32(THETA) ** (-np.arange(half, dtype=np.float32) / np.float32(half))
    cos, sin, zero = np.cos(angle), np.sin(angle), np.zeros(half, np.float32)
    rows = [np.concatenate(r) for r in ((cos, cos), (-sin, zero), (zero, sin))]
    return np.stack([np.tile(r, heads) for r in rows]).astype(np.float32)


def dot(a, b):
    return jnp.dot(a, b, preferred_element_type=F32)


def normed(wide, gain):
    scale = lax.rsqrt(jnp.mean(wide * wide, -1, keepdims=True) + EPS)
    return (wide * scale * gain).astype(BF16)


def layer_kernel(
    x_hbm, k_hbm, v_hbm, ga_hbm, wq_hbm, wo_hbm, gm_hbm, wg_hbm, wu_hbm, wd_hbm, trig_hbm,
    y_ref,
    k_buf, v_buf, wg, wu, wd, wo, x, ga, gm, trig,
    q, o, term, send1, recv1, send2, recv2, h, hid,
    send3, recv3, send4, recv4, states, piece,
    ksem, vsem, qsem, wsem, gsem, usem, dsem, isem,
    s1, r1, s2, r2, s3, r3, s4, r4, s5, r5, s6, r6,
):
    rows, d = x.shape
    width = q.shape[1]
    ff = hid.shape[1]
    half = d // 2
    heads = width // HEAD
    t = lax.axis_index("tp")
    core = lax.rem(t, 2)
    other = 1 - core
    partner = t + 1 - 2 * core
    across = lax.rem(t + 2, 4)
    blocks = rows // SEQS
    per_group = GROUP // SEQS
    groups = rows // GROUP
    nq, nf, nd = d // QCHUNK, ff // FCHUNK, d // DCHUNK
    dh = DCHUNK // 2

    barrier = pltpu.get_barrier_semaphore()
    for peer in (partner, across):
        pl.semaphore_signal(barrier, inc=1, device_id={"tp": peer}, device_id_type=pl.DeviceIdType.MESH)

    def cache_copies(b, slot):
        at = pl.ds(b * SEQS, SEQS)
        return (
            pltpu.make_async_copy(k_hbm.at[at], k_buf.at[slot], ksem.at[slot]),
            pltpu.make_async_copy(v_hbm.at[at], v_buf.at[slot], vsem.at[slot]),
        )

    wq = wg.at[:, pl.ds(0, width)]
    first = [
        pltpu.make_async_copy(x_hbm, x, isem.at[0]),
        pltpu.make_async_copy(ga_hbm, ga, isem.at[1]),
        pltpu.make_async_copy(trig_hbm, trig, isem.at[2]),
    ]
    query_copy = [
        pltpu.make_async_copy(wq_hbm.at[pl.ds(c * QCHUNK, QCHUNK)], wq.at[pl.ds(c * QCHUNK, QCHUNK)], qsem.at[c])
        for c in range(nq)
    ]
    later = [
        pltpu.make_async_copy(gm_hbm, gm, isem.at[3]),
        pltpu.make_async_copy(wo_hbm, wo, wsem),
    ]

    def hidden_units(n):
        return pl.ds(pl.multiple_of(n * FCHUNK, FCHUNK), FCHUNK)

    def out_columns(n):
        return pl.ds(pl.multiple_of(n * DCHUNK, DCHUNK), DCHUNK)

    def gate_copy(n):
        return pltpu.make_async_copy(wg_hbm.at[:, hidden_units(n)], wg.at[:, hidden_units(n)], gsem.at[n])

    def up_copy(n):
        return pltpu.make_async_copy(wu_hbm.at[:, hidden_units(n)], wu.at[:, hidden_units(n)], usem.at[n])

    def down_copy(n):
        return pltpu.make_async_copy(wd_hbm.at[:, out_columns(n)], wd.at[:, out_columns(n)], dsem.at[n])

    for c in first + query_copy:
        c.start()
    for c in cache_copies(0, 0):
        c.start()

    for c in first[:3]:
        c.wait()
    with jax.named_scope('norm_a'):
        a = normed(x[...].astype(F32), ga[...].astype(F32).reshape(1, d))
        states[...] = a
    for c in cache_copies(1, 1):
        c.start()
    for n in range(nq):
        with jax.named_scope('wait_wq'):
            query_copy[n].wait()
        part_q = dot(states[:, n * QCHUNK:(n + 1) * QCHUNK], wg[n * QCHUNK:(n + 1) * QCHUNK, 0:width])
        if n == 0:
            q[...] = part_q
        else:
            q[...] += part_q
    for s in range(2, SLOTS):
        for c in cache_copies(s, s):
            c.start()
    for c in later:
        c.start()
    q0 = q[...].astype(BF16).astype(F32)
    ahead = pltpu.roll(q0, width - HEAD // 2, 1)
    behind = pltpu.roll(q0, HEAD // 2, 1)
    q[...] = (q0 * trig[0:1, :] + ahead * trig[1:2, :] + behind * trig[2:3, :]).astype(BF16).astype(F32)

    lane = lax.broadcasted_iota(jnp.int32, (heads, width), 1)
    top = lax.broadcasted_iota(jnp.int32, (heads, width), 0) * HEAD
    own_head = (lane >= top) & (lane < top + HEAD)

    pl.semaphore_wait(barrier, 2)

    def to(peer, src, dst, ssem, rsem):
        return pltpu.make_async_remote_copy(
            src_ref=src, dst_ref=dst, send_sem=ssem, recv_sem=rsem,
            device_id={"tp": peer}, device_id_type=pl.DeviceIdType.MESH,
        )

    mine = pl.ds(pl.multiple_of(core * half, half), half)
    theirs = pl.ds(pl.multiple_of(other * half, half), half)

    def rows_of(g):
        return pl.ds(pl.multiple_of(g * GROUP, GROUP), GROUP)

    def copy1(g):
        return to(partner, send1.at[rows_of(g)], recv1.at[rows_of(g)], s1.at[g], r1.at[g])

    def copy2(g):
        return to(across, send2.at[rows_of(g)], recv2.at[rows_of(g)], s2.at[g], r2.at[g])

    def copy3(g):
        return to(partner, h.at[rows_of(g), mine], h.at[rows_of(g), mine], s3.at[g], r3.at[g])

    def project(g):
        at = rows_of(g)
        seen = o[at, :].astype(BF16)
        send1[at, :] = dot(seen, wo[:, theirs]).astype(BF16)
        copy1(g).start()
        term[at, :] = dot(seen, wo[:, mine])

    def pair_sum(g):
        at = rows_of(g)
        copy1(g).wait_recv()
        send2[at, :] = (term[at, :] + recv1[at, :].astype(F32)).astype(BF16)
        copy2(g).start()

    def finish(g):
        at = rows_of(g)
        copy2(g).wait_recv()
        total = send2[at, :].astype(F32) + recv2[at, :].astype(F32)
        h[at, mine] = (x[at, mine].astype(F32) + total).astype(BF16)
        copy3(g).start()

    def softmax(scores):
        scores = scores * HEAD**-0.5
        e = jnp.exp(scores - jnp.max(scores, -1, keepdims=True))
        return (e / jnp.sum(e, -1, keepdims=True)).astype(BF16)

    def block(b, carry):
        slot = lax.rem(b, SLOTS)
        kc, vc = cache_copies(b, slot)
        with jax.named_scope('wait_cache'):
            kc.wait()
            vc.wait()
        scores = []
        for i in range(SEQS):
            row = q[pl.ds(b * SEQS + i, 1), :]
            spread = jnp.where(own_head, jnp.broadcast_to(row, (heads, width)), 0.0).astype(BF16)
            scores.append(dot(spread, k_buf[slot, i]))
        for i in range(SEQS):
            weights = softmax(scores[i])
            out = lax.dot_general(weights, v_buf[slot, i], NT, preferred_element_type=F32)
            o[pl.ds(b * SEQS + i, 1), :] = jnp.sum(jnp.where(own_head, out, 0.0), 0, keepdims=True)

        @pl.when(b + SLOTS < blocks)
        def _():
            for c in cache_copies(b + SLOTS, slot):
                c.start()

        for n in range(SLOTS):
            @pl.when(b == blocks - SLOTS + n)
            def _():
                gate_copy(n).start()
                up_copy(n).start()

        g = lax.div(b, per_group)
        step = lax.rem(b, per_group)

        @pl.when(b == per_group - 1)
        def _():
            later[1].wait()

        @pl.when(step == per_group - 1)
        def _():
            with jax.named_scope('project'):
                project(g)

        @pl.when((step == 0) & (b > 0))
        def _():
            with jax.named_scope('pair_sum'):
                pair_sum(g - 1)

        @pl.when((step == 3) & (b > per_group))
        def _():
            with jax.named_scope('finish'):
                finish(g - 1)

        return carry

    lax.fori_loop(0, blocks, block, 0)
    for n in range(SLOTS, nf):
        gate_copy(n).start()
        up_copy(n).start()

    with jax.named_scope('pair_sum'):
        pair_sum(groups - 1)
    with jax.named_scope('finish'):
        finish(groups - 1)
    later[0].wait()
    with jax.named_scope('wait_h'):
        for g in range(groups):
            copy3(g).wait_recv()
    for n in range(nd):
        down_copy(n).start()
    with jax.named_scope('norm_m'):
        states[...] = normed(h[...].astype(F32), gm[...].astype(F32).reshape(1, d))

    def gate_up(n, carry):
        at = hidden_units(n)
        with jax.named_scope('wait_gate_up'):
            gate_copy(n).wait()
            up_copy(n).wait()
        gate = dot(states[...], wg[:, at])
        up = dot(states[...], wu[:, at])
        hid[:, at] = (gate * jax.nn.sigmoid(gate) * up).astype(BF16)
        return carry

    lax.fori_loop(0, nf, gate_up, 0)

    def columns(n, which):
        return pl.ds(pl.multiple_of(n * DCHUNK + which * dh, dh), dh)

    def part(n):
        return pl.ds(pl.multiple_of(n * dh, dh), dh)

    def copy4(n):
        return to(partner, send3.at[:, part(n)], recv3.at[:, part(n)], s4.at[n], r4.at[n])

    def copy5(n):
        return to(across, send4.at[:, part(n)], recv4.at[:, part(n)], s5.at[n], r5.at[n])

    def copy6(n):
        return to(partner, y_ref.at[:, columns(n, core)], y_ref.at[:, columns(n, core)], s6.at[n], r6.at[n])

    def down(n):
        with jax.named_scope('wait_down'):
            down_copy(n).wait()
        piece[...] = dot(hid[...], wd[:, out_columns(n)])
        send3[:, part(n)] = piece[:, pl.ds(pl.multiple_of(other * dh, dh), dh)].astype(BF16)
        copy4(n).start()
        term[:, part(n)] = piece[:, pl.ds(pl.multiple_of(core * dh, dh), dh)]

    def down_pair(n):
        with jax.named_scope('wait_pair'):
            copy4(n).wait_recv()
        send4[:, part(n)] = (term[:, part(n)] + recv3[:, part(n)].astype(F32)).astype(BF16)
        copy5(n).start()

    def down_finish(n, carry):
        with jax.named_scope('wait_across'):
            copy5(n).wait_recv()
        total = send4[:, part(n)].astype(F32) + recv4[:, part(n)].astype(F32)
        y_ref[:, columns(n, core)] = (h[:, columns(n, core)].astype(F32) + total).astype(BF16)
        copy6(n).start()
        return carry

    def down_step(n, carry):
        @pl.when(n < nd)
        def _():
            down(n)

        @pl.when(n >= LAG)
        def _():
            down_pair(n - LAG)

        return carry

    lax.fori_loop(0, nd + LAG, down_step, 0)
    lax.fori_loop(0, nd, down_finish, 0)
    with jax.named_scope('last_waits'):
        for g in range(groups):
            copy1(g).wait_send()
            copy2(g).wait_send()
            copy3(g).wait_send()
        for n in range(nd):
            copy4(n).wait_send()
            copy5(n).wait_send()
            copy6(n).wait()


def solution(mesh):
    def step(x, k_cache, v_cache, gain_a, wq, wo, gain_m, w_gate, w_up, w_down):
        rows, d = x.shape
        cache, heads = k_cache.shape[1:3]
        width = heads * HEAD
        ff = w_gate.shape[1]
        turned_cache = [c.transpose(0, 2, 3, 1).reshape(rows, width, cache) for c in (k_cache, v_cache)]
        trig = jnp.asarray(rotary_table(heads, HEAD, cache - 1))
        half, groups, nf, nd = d // 2, rows // GROUP, ff // FCHUNK, d // DCHUNK
        dma = pltpu.SemaphoreType.DMA
        return pl.pallas_call(
            layer_kernel,
            out_shape=jax.ShapeDtypeStruct((rows, d), BF16),
            in_specs=[pl.BlockSpec(memory_space=pl.ANY)] * 11,
            out_specs=pl.BlockSpec(memory_space=pltpu.VMEM),
            scratch_shapes=[
                pltpu.VMEM((SLOTS, SEQS, width, cache), BF16),
                pltpu.VMEM((SLOTS, SEQS, width, cache), BF16),
                pltpu.VMEM((d, ff), BF16),
                pltpu.VMEM((d, ff), BF16),
                pltpu.VMEM((ff, d), BF16),
                pltpu.VMEM((width, d), BF16),
                pltpu.VMEM((rows, d), BF16),
                pltpu.VMEM((d,), BF16),
                pltpu.VMEM((d,), BF16),
                pltpu.VMEM((3, width), F32),
                pltpu.VMEM((rows, width), F32),
                pltpu.VMEM((rows, width), F32),
                pltpu.VMEM((rows, half), F32),
                pltpu.VMEM((rows, half), BF16),
                pltpu.VMEM((rows, half), BF16),
                pltpu.VMEM((rows, half), BF16),
                pltpu.VMEM((rows, half), BF16),
                pltpu.VMEM((rows, d), BF16),
                pltpu.VMEM((rows, ff), BF16),
                pltpu.VMEM((rows, half), BF16),
                pltpu.VMEM((rows, half), BF16),
                pltpu.VMEM((rows, half), BF16),
                pltpu.VMEM((rows, half), BF16),
                pltpu.VMEM((rows, d), BF16),
                pltpu.VMEM((rows, DCHUNK), F32),
                dma((SLOTS,)), dma((SLOTS,)), dma((d // QCHUNK,)), dma, dma((nf,)), dma((nf,)), dma((nd,)), dma((4,)),
                *[dma((groups,)) for _ in range(6)],
                *[dma((nd,)) for _ in range(6)],
            ],
            compiler_params=pltpu.CompilerParams(
                collective_id=0, has_side_effects=True, vmem_limit_bytes=67043328
            ),
            name="decode_layer",
        )(x, *turned_cache, gain_a, wq, wo, gain_m, w_gate, w_up, w_down, trig)

    states, cache, columns, rows_of = P("dp", None), P("dp", None, "tp", None), P(None, "tp"), P("tp", None)
    return jax.shard_map(
        step,
        mesh=mesh,
        in_specs=(states, cache, cache, P(None), columns, rows_of, P(None), columns, columns, rows_of),
        out_specs=states,
        check_vma=False,
    )
```

```python
import jax
import jax.numpy as jnp
import numpy as np
from jax import lax
from jax.experimental import pallas as pl
from jax.experimental.pallas import tpu as pltpu
from jax.sharding import PartitionSpec as P

HEAD = 96
THETA = 10000
EPS = 1e-6
EARLY = 3
SLOTS = 5
GROUP = 16
QCHUNK = 768
FCHUNK = 512
FSTEP = 1024
PADDED = 128
DCHUNK = 512
LAG = 2

F32, BF16 = jnp.float32, jnp.bfloat16
NT = (((1,), (1,)), ((), ()))


def rotary_table(heads, head, place):
    half = head // 2
    angle = np.float32(place) * np.float32(THETA) ** (-np.arange(half, dtype=np.float32) / np.float32(half))
    cos, sin, zero = np.cos(angle), np.sin(angle), np.zeros(half, np.float32)
    rows = [np.concatenate(r) for r in ((cos, cos), (-sin, zero), (zero, sin))]
    return np.stack([np.tile(r, heads) for r in rows]).astype(np.float32)


def dot(a, b):
    return jnp.dot(a, b, preferred_element_type=F32)


def normed(wide, gain):
    scale = lax.rsqrt(jnp.mean(wide * wide, -1, keepdims=True) + EPS)
    return (wide * scale * gain).astype(BF16)


def layer_kernel(
    x_hbm, k_hbm, v_hbm, ga_hbm, wq_hbm, wo_hbm, gm_hbm, wg_hbm, wu_hbm, wd_hbm, trig_hbm,
    y_hbm,
    k_buf, v_buf, wg, wu, wd, wo, x, ga, gm, trig,
    q, o, term, send1, recv1, send2, recv2, h, hid,
    send3, recv3, send4, recv4, states, piece, y_ref,
    ksem, vsem, qsem, wsem, gsem, usem, dsem, isem,
    s1, r1, s2, r2, s3, r3, s4, r4, s5, r5, s6, r6, ysem,
):
    rows, d = x.shape
    width = q.shape[1]
    ff = hid.shape[1]
    half = d // 2
    heads = width // HEAD
    t = lax.axis_index("tp")
    core = lax.rem(t, 2)
    other = 1 - core
    partner = t + 1 - 2 * core
    across = lax.rem(t + 2, 4)
    groups = rows // GROUP
    nq, nf, nd = d // QCHUNK, ff // FCHUNK, d // DCHUNK
    dh = DCHUNK // 2

    barrier = pltpu.get_barrier_semaphore()
    for peer in (partner, across):
        pl.semaphore_signal(barrier, inc=1, device_id={"tp": peer}, device_id_type=pl.DeviceIdType.MESH)

    def key_copy(i):
        slot = lax.rem(i, SLOTS)
        return pltpu.make_async_copy(k_hbm.at[i], k_buf.at[slot], ksem.at[slot])

    def value_copy(i):
        slot = lax.rem(i, SLOTS)
        return pltpu.make_async_copy(v_hbm.at[i], v_buf.at[slot], vsem.at[slot])

    wq = wg.at[:, pl.ds(0, width)]
    first = [
        pltpu.make_async_copy(x_hbm, x, isem.at[0]),
        pltpu.make_async_copy(ga_hbm, ga, isem.at[1]),
        pltpu.make_async_copy(trig_hbm, trig, isem.at[2]),
    ]
    query_copy = [
        pltpu.make_async_copy(wq_hbm.at[pl.ds(c * QCHUNK, QCHUNK)], wq.at[pl.ds(c * QCHUNK, QCHUNK)], qsem.at[c])
        for c in range(nq)
    ]
    later = [
        pltpu.make_async_copy(gm_hbm, gm, isem.at[3]),
        pltpu.make_async_copy(wo_hbm, wo, wsem),
    ]

    def hidden_units(n):
        return pl.ds(pl.multiple_of(n * FCHUNK, FCHUNK), FCHUNK)

    def out_columns(n):
        return pl.ds(pl.multiple_of(n * DCHUNK, DCHUNK), DCHUNK)

    def gate_copy(n):
        return pltpu.make_async_copy(wg_hbm.at[:, hidden_units(n)], wg.at[:, hidden_units(n)], gsem.at[n])

    def up_copy(n):
        return pltpu.make_async_copy(wu_hbm.at[:, hidden_units(n)], wu.at[:, hidden_units(n)], usem.at[n])

    def weight_copy(n):
        return (up_copy if n % 2 else gate_copy)(n // 2)

    def down_copy(n):
        return pltpu.make_async_copy(wd_hbm.at[:, out_columns(n)], wd.at[:, out_columns(n)], dsem.at[n])

    for c in first + query_copy:
        c.start()
    for i in range(2):
        key_copy(i).start()
        value_copy(i).start()

    for c in first[:3]:
        c.wait()
    with jax.named_scope('norm_a'):
        a = normed(x[...].astype(F32), ga[...].astype(F32).reshape(1, d))
        states[0:rows, :] = a
        states[rows:PADDED, :] = jnp.zeros((PADDED - rows, d), BF16)
    for i in range(2, 4):
        key_copy(i).start()
        value_copy(i).start()
    for n in range(nq):
        with jax.named_scope('wait_wq'):
            query_copy[n].wait()
        part_q = dot(states[0:rows, n * QCHUNK:(n + 1) * QCHUNK], wg[n * QCHUNK:(n + 1) * QCHUNK, 0:width])
        if n == 0:
            q[...] = part_q
        else:
            q[...] += part_q
    for i in range(4, SLOTS):
        key_copy(i).start()
        value_copy(i).start()
    for c in later:
        c.start()
    q0 = q[...].astype(BF16).astype(F32)
    ahead = pltpu.roll(q0, width - HEAD // 2, 1)
    behind = pltpu.roll(q0, HEAD // 2, 1)
    q[...] = (q0 * trig[0:1, :] + ahead * trig[1:2, :] + behind * trig[2:3, :]).astype(BF16).astype(F32)

    lane = lax.broadcasted_iota(jnp.int32, (heads, width), 1)
    top = lax.broadcasted_iota(jnp.int32, (heads, width), 0) * HEAD
    own_head = (lane >= top) & (lane < top + HEAD)

    pl.semaphore_wait(barrier, 2)

    def to(peer, src, dst, ssem, rsem):
        return pltpu.make_async_remote_copy(
            src_ref=src, dst_ref=dst, send_sem=ssem, recv_sem=rsem,
            device_id={"tp": peer}, device_id_type=pl.DeviceIdType.MESH,
        )

    mine = pl.ds(pl.multiple_of(core * half, half), half)
    theirs = pl.ds(pl.multiple_of(other * half, half), half)

    def rows_of(g):
        return pl.ds(pl.multiple_of(g * GROUP, GROUP), GROUP)

    def copy1(g):
        return to(partner, send1.at[rows_of(g)], recv1.at[rows_of(g)], s1.at[g], r1.at[g])

    def copy2(g):
        return to(across, send2.at[rows_of(g)], recv2.at[rows_of(g)], s2.at[g], r2.at[g])

    def copy3(g):
        return to(partner, h.at[rows_of(g), mine], h.at[rows_of(g), mine], s3.at[g], r3.at[g])

    def project(g):
        at = rows_of(g)
        seen = o[at, :].astype(BF16)
        send1[at, :] = dot(seen, wo[:, theirs]).astype(BF16)
        copy1(g).start()
        term[at, :] = dot(seen, wo[:, mine])

    def pair_sum(g):
        at = rows_of(g)
        copy1(g).wait_recv()
        send2[at, :] = (term[at, :] + recv1[at, :].astype(F32)).astype(BF16)
        copy2(g).start()

    def finish(g):
        at = rows_of(g)
        copy2(g).wait_recv()
        total = send2[at, :].astype(F32) + recv2[at, :].astype(F32)
        h[at, mine] = (x[at, mine].astype(F32) + total).astype(BF16)
        copy3(g).start()

    def softmax(scores):
        scores = scores * HEAD**-0.5
        e = jnp.exp(scores - jnp.max(scores, -1, keepdims=True))
        return (e / jnp.sum(e, -1, keepdims=True)).astype(BF16)

    def scores_of(i):
        row = q[pl.ds(i, 1), :]
        spread = jnp.where(own_head, jnp.broadcast_to(row, (heads, width)), 0.0).astype(BF16)
        return dot(spread, k_buf[lax.rem(i, SLOTS)])

    def add_values(i, weights):
        out = lax.dot_general(weights, v_buf[lax.rem(i, SLOTS)], NT, preferred_element_type=F32)
        o[pl.ds(i, 1), :] = jnp.sum(jnp.where(own_head, out, 0.0), 0, keepdims=True)

    key_copy(0).wait()
    weights = softmax(scores_of(0))
    key_copy(SLOTS).start()

    def sequence(i, weights):
        with jax.named_scope('wait_cache'):
            key_copy(i + 1).wait()
            value_copy(i).wait()
        scores = scores_of(i + 1)
        add_values(i, weights)
        weights = softmax(scores)

        @pl.when(i + 1 + SLOTS < rows)
        def _():
            key_copy(i + 1 + SLOTS).start()

        @pl.when(i + SLOTS < rows)
        def _():
            value_copy(i + SLOTS).start()

        for n in range(EARLY):
            @pl.when(i == rows - 1 - EARLY + n)
            def _():
                weight_copy(n).start()

        g = lax.div(i, GROUP)
        step = lax.rem(i, GROUP)

        @pl.when(i == GROUP - 1)
        def _():
            later[1].wait()

        @pl.when(step == GROUP - 1)
        def _():
            with jax.named_scope('project'):
                project(g)

        @pl.when((step == 1) & (i > GROUP))
        def _():
            with jax.named_scope('pair_sum'):
                pair_sum(g - 1)

        @pl.when((step == 6) & (i > GROUP))
        def _():
            with jax.named_scope('finish'):
                finish(g - 1)

        return weights

    weights = lax.fori_loop(0, rows - 1, sequence, weights)
    for n in range(EARLY, 2 * nf):
        weight_copy(n).start()
    with jax.named_scope('last_cache'):
        value_copy(rows - 1).wait()
    add_values(rows - 1, weights)
    with jax.named_scope('project'):
        project(groups - 1)

    with jax.named_scope('pair_sum'):
        pair_sum(groups - 1)
    with jax.named_scope('finish'):
        finish(groups - 1)
    later[0].wait()
    with jax.named_scope('wait_h'):
        for g in range(groups):
            copy3(g).wait_recv()
    for n in range(nd):
        down_copy(n).start()
    with jax.named_scope('norm_m'):
        states[0:rows, :] = normed(h[...].astype(F32), gm[...].astype(F32).reshape(1, d))

    for n in range(ff // FSTEP):
        at = pl.ds(n * FSTEP, FSTEP)
        with jax.named_scope('wait_gate_up'):
            for m in range(n * FSTEP // FCHUNK, (n + 1) * FSTEP // FCHUNK):
                gate_copy(m).wait()
                up_copy(m).wait()
        gate = dot(states[...], wg[:, at])[:rows]
        up = dot(states[...], wu[:, at])[:rows]
        hid[:, at] = (gate * jax.nn.sigmoid(gate) * up).astype(BF16)

    def columns(n, which):
        return pl.ds(pl.multiple_of(n * DCHUNK + which * dh, dh), dh)

    def part(n):
        return pl.ds(pl.multiple_of(n * dh, dh), dh)

    def copy4(n):
        return to(partner, send3.at[:, part(n)], recv3.at[:, part(n)], s4.at[n], r4.at[n])

    def copy5(n):
        return to(across, send4.at[:, part(n)], recv4.at[:, part(n)], s5.at[n], r5.at[n])

    def copy6(n):
        return to(partner, y_ref.at[:, columns(n, core)], y_ref.at[:, columns(n, core)], s6.at[n], r6.at[n])

    def out_copy(n, which, i):
        at = columns(n, which)
        return pltpu.make_async_copy(y_ref.at[:, at], y_hbm.at[:, at], ysem.at[i, n])

    def down(n):
        with jax.named_scope('wait_down'):
            down_copy(n).wait()
        piece[...] = dot(hid[...], wd[:, out_columns(n)])
        send3[:, part(n)] = piece[:, pl.ds(pl.multiple_of(other * dh, dh), dh)].astype(BF16)
        copy4(n).start()
        term[:, part(n)] = piece[:, pl.ds(pl.multiple_of(core * dh, dh), dh)]

    def down_pair(n):
        with jax.named_scope('wait_pair'):
            copy4(n).wait_recv()
        send4[:, part(n)] = (term[:, part(n)] + recv3[:, part(n)].astype(F32)).astype(BF16)
        copy5(n).start()

    def down_finish(n, carry):
        with jax.named_scope('wait_across'):
            copy5(n).wait_recv()
        total = send4[:, part(n)].astype(F32) + recv4[:, part(n)].astype(F32)
        y_ref[:, columns(n, core)] = (h[:, columns(n, core)].astype(F32) + total).astype(BF16)
        copy6(n).start()
        out_copy(n, core, 0).start()
        return carry

    def down_step(n, carry):
        @pl.when(n < nd)
        def _():
            down(n)

        @pl.when(n >= LAG)
        def _():
            down_pair(n - LAG)

        return carry

    lax.fori_loop(0, nd + LAG, down_step, 0)
    lax.fori_loop(0, nd, down_finish, 0)
    with jax.named_scope('send_waits'):
        for g in range(groups):
            copy1(g).wait_send()
            copy2(g).wait_send()
            copy3(g).wait_send()
        for n in range(nd):
            copy4(n).wait_send()
            copy5(n).wait_send()
    with jax.named_scope('wait_y'):
        for n in range(nd):
            copy6(n).wait_recv()
            out_copy(n, other, 1).start()
    with jax.named_scope('wait_out'):
        for n in range(nd):
            copy6(n).wait_send()
            out_copy(n, core, 0).wait()
            out_copy(n, other, 1).wait()


def solution(mesh):
    def step(x, k_cache, v_cache, gain_a, wq, wo, gain_m, w_gate, w_up, w_down):
        rows, d = x.shape
        cache, heads = k_cache.shape[1:3]
        width = heads * HEAD
        ff = w_gate.shape[1]
        turned_cache = [c.transpose(0, 2, 3, 1).reshape(rows, width, cache) for c in (k_cache, v_cache)]
        trig = jnp.asarray(rotary_table(heads, HEAD, cache - 1))
        half, groups, nf, nd = d // 2, rows // GROUP, ff // FCHUNK, d // DCHUNK
        dma = pltpu.SemaphoreType.DMA
        return pl.pallas_call(
            layer_kernel,
            out_shape=jax.ShapeDtypeStruct((rows, d), BF16),
            in_specs=[pl.BlockSpec(memory_space=pl.ANY)] * 11,
            out_specs=pl.BlockSpec(memory_space=pl.ANY),
            scratch_shapes=[
                pltpu.VMEM((SLOTS, width, cache), BF16),
                pltpu.VMEM((SLOTS, width, cache), BF16),
                pltpu.VMEM((d, ff), BF16),
                pltpu.VMEM((d, ff), BF16),
                pltpu.VMEM((ff, d), BF16),
                pltpu.VMEM((width, d), BF16),
                pltpu.VMEM((rows, d), BF16),
                pltpu.VMEM((d,), BF16),
                pltpu.VMEM((d,), BF16),
                pltpu.VMEM((3, width), F32),
                pltpu.VMEM((rows, width), F32),
                pltpu.VMEM((rows, width), F32),
                pltpu.VMEM((rows, half), F32),
                pltpu.VMEM((rows, half), BF16),
                pltpu.VMEM((rows, half), BF16),
                pltpu.VMEM((rows, half), BF16),
                pltpu.VMEM((rows, half), BF16),
                pltpu.VMEM((rows, d), BF16),
                pltpu.VMEM((rows, ff), BF16),
                pltpu.VMEM((rows, half), BF16),
                pltpu.VMEM((rows, half), BF16),
                pltpu.VMEM((rows, half), BF16),
                pltpu.VMEM((rows, half), BF16),
                pltpu.VMEM((PADDED, d), BF16),
                pltpu.VMEM((rows, DCHUNK), F32),
                pltpu.VMEM((rows, d), BF16),
                dma((SLOTS,)), dma((SLOTS,)), dma((d // QCHUNK,)), dma, dma((nf,)), dma((nf,)), dma((nd,)), dma((4,)),
                *[dma((groups,)) for _ in range(6)],
                *[dma((nd,)) for _ in range(6)],
                dma((2, nd)),
            ],
            compiler_params=pltpu.CompilerParams(
                collective_id=0, has_side_effects=True, vmem_limit_bytes=67043328
            ),
            name="decode_layer",
        )(x, *turned_cache, gain_a, wq, wo, gain_m, w_gate, w_up, w_down, trig)

    states, cache, columns, rows_of = P("dp", None), P("dp", None, "tp", None), P(None, "tp"), P("tp", None)
    return jax.shard_map(
        step,
        mesh=mesh,
        in_specs=(states, cache, cache, P(None), columns, rows_of, P(None), columns, columns, rows_of),
        out_specs=states,
        check_vma=False,
    )
```

```python
import jax
import jax.numpy as jnp
import numpy as np
from jax import lax
from jax.experimental import pallas as pl
from jax.experimental.pallas import tpu as pltpu
from jax.sharding import PartitionSpec as P

HEAD = 96
THETA = 10000
EPS = 1e-6
VMEM_LIMIT = 66_500_000
EARLY = 3
SLOTS = 5
GROUP = 16
QCHUNK = 768
FCHUNK = 512
FSTEP = 1024
PADDED = 128
DCHUNK = 512
LAG = 1

F32, BF16 = jnp.float32, jnp.bfloat16
NT = (((1,), (1,)), ((), ()))


def rotary_table(heads, head, place):
    half = head // 2
    angle = np.float32(place) * np.float32(THETA) ** (-np.arange(half, dtype=np.float32) / np.float32(half))
    cos, sin, zero = np.cos(angle), np.sin(angle), np.zeros(half, np.float32)
    rows = [np.concatenate(r) for r in ((cos, cos), (-sin, zero), (zero, sin))]
    return np.stack([np.tile(r, heads) for r in rows]).astype(np.float32)


def dot(a, b):
    return jnp.dot(a, b, preferred_element_type=F32)


def normed(wide, gain):
    scale = lax.rsqrt(jnp.mean(wide * wide, -1, keepdims=True) + EPS)
    return (wide * scale * gain).astype(BF16)


def layer_kernel(
    x_hbm, k_hbm, v_hbm, ga_hbm, wq_hbm, wo_hbm, gm_hbm, wg_hbm, wu_hbm, wd_hbm, trig_hbm,
    y_ref,
    k_buf, v_buf, wg, wu, wd, wo, x, ga, gm, trig,
    q, o, term, send1, recv1, send2, recv2, h, hid,
    send3, recv3, send4, recv4, states, piece,
    ksem, vsem, qsem, wsem, gsem, usem, dsem, isem,
    s1, r1, s2, r2, s3, r3, s4, r4, s5, r5, s6, r6,
):
    rows, d = x.shape
    width = q.shape[1]
    ff = hid.shape[1]
    half = d // 2
    heads = width // HEAD
    t = lax.axis_index("tp")
    core = lax.rem(t, 2)
    other = 1 - core
    partner = t + 1 - 2 * core
    across = lax.rem(t + 2, 4)
    groups = rows // GROUP
    nq, nf, nd = d // QCHUNK, ff // FCHUNK, d // DCHUNK
    dh = DCHUNK // 2

    barrier = pltpu.get_barrier_semaphore()
    for peer in (partner, across):
        pl.semaphore_signal(barrier, inc=1, device_id={"tp": peer}, device_id_type=pl.DeviceIdType.MESH)

    def key_copy(i):
        slot = lax.rem(i, SLOTS)
        return pltpu.make_async_copy(k_hbm.at[i], k_buf.at[slot], ksem.at[slot])

    def value_copy(i):
        slot = lax.rem(i, SLOTS)
        return pltpu.make_async_copy(v_hbm.at[i], v_buf.at[slot], vsem.at[slot])

    wq = wg.at[:, pl.ds(0, width)]
    first = [
        pltpu.make_async_copy(x_hbm, x, isem.at[0]),
        pltpu.make_async_copy(ga_hbm, ga, isem.at[1]),
        pltpu.make_async_copy(trig_hbm, trig, isem.at[2]),
    ]
    query_copy = [
        pltpu.make_async_copy(wq_hbm.at[pl.ds(c * QCHUNK, QCHUNK)], wq.at[pl.ds(c * QCHUNK, QCHUNK)], qsem.at[c])
        for c in range(nq)
    ]
    later = [
        pltpu.make_async_copy(gm_hbm, gm, isem.at[3]),
        pltpu.make_async_copy(wo_hbm, wo, wsem),
    ]

    def hidden_units(n):
        return pl.ds(pl.multiple_of(n * FCHUNK, FCHUNK), FCHUNK)

    def out_columns(n):
        return pl.ds(pl.multiple_of(n * DCHUNK, DCHUNK), DCHUNK)

    def gate_copy(n):
        return pltpu.make_async_copy(wg_hbm.at[:, hidden_units(n)], wg.at[:, hidden_units(n)], gsem.at[n * FCHUNK // FSTEP])

    def up_copy(n):
        return pltpu.make_async_copy(wu_hbm.at[:, hidden_units(n)], wu.at[:, hidden_units(n)], usem.at[n * FCHUNK // FSTEP])

    def weight_copy(n):
        return (up_copy if n % 2 else gate_copy)(n // 2)

    def down_copy(n):
        return pltpu.make_async_copy(wd_hbm.at[:, out_columns(n)], wd.at[:, out_columns(n)], dsem.at[n])

    for c in first + query_copy:
        c.start()
    for i in range(2):
        key_copy(i).start()
        value_copy(i).start()

    for c in first[:3]:
        c.wait()
    with jax.named_scope('norm_a'):
        a = normed(x[...].astype(F32), ga[...].astype(F32).reshape(1, d))
        states[0:rows, :] = a
        states[rows:PADDED, :] = jnp.zeros((PADDED - rows, d), BF16)
    for i in range(2, 4):
        key_copy(i).start()
        value_copy(i).start()
    for n in range(nq):
        with jax.named_scope('wait_wq'):
            query_copy[n].wait()
        part_q = dot(states[0:rows, n * QCHUNK:(n + 1) * QCHUNK], wg[n * QCHUNK:(n + 1) * QCHUNK, 0:width])
        if n == 0:
            q[...] = part_q
        else:
            q[...] += part_q
    for i in range(4, SLOTS):
        key_copy(i).start()
        value_copy(i).start()
    for c in later:
        c.start()
    q0 = q[...].astype(BF16).astype(F32)
    ahead = pltpu.roll(q0, width - HEAD // 2, 1)
    behind = pltpu.roll(q0, HEAD // 2, 1)
    q[...] = (q0 * trig[0:1, :] + ahead * trig[1:2, :] + behind * trig[2:3, :]).astype(BF16).astype(F32)

    lane = lax.broadcasted_iota(jnp.int32, (heads, width), 1)
    top = lax.broadcasted_iota(jnp.int32, (heads, width), 0) * HEAD
    own_head = (lane >= top) & (lane < top + HEAD)

    pl.semaphore_wait(barrier, 2)

    def to(peer, src, dst, ssem, rsem):
        return pltpu.make_async_remote_copy(
            src_ref=src, dst_ref=dst, send_sem=ssem, recv_sem=rsem,
            device_id={"tp": peer}, device_id_type=pl.DeviceIdType.MESH,
        )

    mine = pl.ds(pl.multiple_of(core * half, half), half)
    theirs = pl.ds(pl.multiple_of(other * half, half), half)

    def rows_of(g):
        return pl.ds(pl.multiple_of(g * GROUP, GROUP), GROUP)

    def copy1(g):
        return to(partner, send1.at[rows_of(g)], recv1.at[rows_of(g)], s1, r1.at[g])

    def copy2(g):
        return to(across, send2.at[rows_of(g)], recv2.at[rows_of(g)], s2, r2.at[g])

    def copy3(g):
        return to(partner, h.at[rows_of(g), mine], h.at[rows_of(g), mine], s3, r3)

    def project(g):
        at = rows_of(g)
        seen = o[at, :].astype(BF16)
        send1[at, :] = dot(seen, wo[:, theirs]).astype(BF16)
        copy1(g).start()
        term[at, :] = dot(seen, wo[:, mine])

    def pair_sum(g):
        at = rows_of(g)
        copy1(g).wait_recv()
        send2[at, :] = (term[at, :] + recv1[at, :].astype(F32)).astype(BF16)
        copy2(g).start()

    def finish(g):
        at = rows_of(g)
        copy2(g).wait_recv()
        total = send2[at, :].astype(F32) + recv2[at, :].astype(F32)
        h[at, mine] = (x[at, mine].astype(F32) + total).astype(BF16)
        copy3(g).start()

    def softmax(scores):
        scores = scores * HEAD**-0.5
        e = jnp.exp(scores - jnp.max(scores, -1, keepdims=True))
        return (e / jnp.sum(e, -1, keepdims=True)).astype(BF16)

    def scores_of(i):
        row = q[pl.ds(i, 1), :]
        spread = jnp.where(own_head, jnp.broadcast_to(row, (heads, width)), 0.0).astype(BF16)
        return dot(spread, k_buf[lax.rem(i, SLOTS)])

    def add_values(i, weights):
        out = lax.dot_general(weights, v_buf[lax.rem(i, SLOTS)], NT, preferred_element_type=F32)
        o[pl.ds(i, 1), :] = jnp.sum(jnp.where(own_head, out, 0.0), 0, keepdims=True)

    key_copy(0).wait()
    weights = softmax(scores_of(0))
    key_copy(SLOTS).start()

    def sequence(i, weights):
        with jax.named_scope('wait_cache'):
            key_copy(i + 1).wait()
            value_copy(i).wait()
        scores = scores_of(i + 1)
        add_values(i, weights)
        weights = softmax(scores)

        @pl.when(i + 1 + SLOTS < rows)
        def _():
            key_copy(i + 1 + SLOTS).start()

        @pl.when(i + SLOTS < rows)
        def _():
            value_copy(i + SLOTS).start()

        for n in range(EARLY):
            @pl.when(i == rows - 1 - EARLY + n)
            def _():
                weight_copy(n).start()

        g = lax.div(i, GROUP)
        step = lax.rem(i, GROUP)

        @pl.when(i == GROUP - 1)
        def _():
            later[1].wait()

        @pl.when(step == GROUP - 1)
        def _():
            with jax.named_scope('project'):
                project(g)

        @pl.when((step == 1) & (i > GROUP))
        def _():
            with jax.named_scope('pair_sum'):
                pair_sum(g - 1)

        @pl.when((step == 6) & (i > GROUP))
        def _():
            with jax.named_scope('finish'):
                finish(g - 1)

        return weights

    weights = lax.fori_loop(0, rows - 1, sequence, weights)
    for n in range(EARLY, 2 * nf):
        weight_copy(n).start()
    with jax.named_scope('last_cache'):
        value_copy(rows - 1).wait()
    add_values(rows - 1, weights)
    with jax.named_scope('project'):
        project(groups - 1)

    with jax.named_scope('pair_sum'):
        pair_sum(groups - 1)
    with jax.named_scope('finish'):
        finish(groups - 1)
    later[0].wait()
    with jax.named_scope('wait_h'):
        to(partner, h.at[:, mine], h.at[:, mine], s3, r3).wait_recv()
    for n in range(nd):
        down_copy(n).start()
    with jax.named_scope('norm_m'):
        states[0:rows, :] = normed(h[...].astype(F32), gm[...].astype(F32).reshape(1, d))

    for n in range(ff // FSTEP):
        at = pl.ds(n * FSTEP, FSTEP)
        with jax.named_scope('wait_gate_up'):
            pltpu.make_async_copy(wg_hbm.at[:, at], wg.at[:, at], gsem.at[n]).wait()
            pltpu.make_async_copy(wu_hbm.at[:, at], wu.at[:, at], usem.at[n]).wait()
        gate = dot(states[...], wg[:, at])[:rows]
        up = dot(states[...], wu[:, at])[:rows]
        hid[:, at] = (gate * jax.nn.sigmoid(gate) * up).astype(BF16)

    def columns(n, which):
        return pl.ds(pl.multiple_of(n * DCHUNK + which * dh, dh), dh)

    def part(n):
        return pl.ds(pl.multiple_of(n * dh, dh), dh)

    def copy4(n):
        return to(partner, send3.at[:, part(n)], recv3.at[:, part(n)], s4, r4.at[n])

    def copy5(n):
        return to(across, send4.at[:, part(n)], recv4.at[:, part(n)], s5, r5.at[n])

    def copy6(n):
        return to(partner, y_ref.at[:, columns(n, core)], y_ref.at[:, columns(n, core)], s6, r6)

    def down(n):
        with jax.named_scope('wait_down'):
            down_copy(n).wait()
        piece[...] = dot(hid[...], wd[:, out_columns(n)])
        send3[:, part(n)] = piece[:, pl.ds(pl.multiple_of(other * dh, dh), dh)].astype(BF16)
        copy4(n).start()
        term[:, part(n)] = piece[:, pl.ds(pl.multiple_of(core * dh, dh), dh)]

    def down_pair(n):
        with jax.named_scope('wait_pair'):
            copy4(n).wait_recv()
        send4[:, part(n)] = (term[:, part(n)] + recv3[:, part(n)].astype(F32)).astype(BF16)
        copy5(n).start()

    def down_finish(n, carry):
        with jax.named_scope('wait_across'):
            copy5(n).wait_recv()
        total = send4[:, part(n)].astype(F32) + recv4[:, part(n)].astype(F32)
        y_ref[:, columns(n, core)] = (h[:, columns(n, core)].astype(F32) + total).astype(BF16)
        copy6(n).start()
        return carry

    def down_step(n, carry):
        @pl.when(n < nd)
        def _():
            down(n)

        @pl.when(n >= LAG)
        def _():
            down_pair(n - LAG)

        return carry

    lax.fori_loop(0, nd + LAG, down_step, 0)
    lax.fori_loop(0, nd, down_finish, 0)
    with jax.named_scope('send_waits'):
        for send, recv, ssem, rsem in (
            (send1, recv1, s1, r1.at[0]), (send2, recv2, s2, r2.at[0]), (send3, recv3, s4, r4.at[0]), (send4, recv4, s5, r5.at[0]),
        ):
            to(partner, send, recv, ssem, rsem).wait_send()
        to(partner, h.at[:, mine], h.at[:, mine], s3, r3).wait_send()
    with jax.named_scope('wait_y'):
        to(partner, y_ref.at[:, mine], y_ref.at[:, mine], s6, r6).wait()


def solution(mesh):
    def step(x, k_cache, v_cache, gain_a, wq, wo, gain_m, w_gate, w_up, w_down):
        rows, d = x.shape
        cache, heads = k_cache.shape[1:3]
        width = heads * HEAD
        ff = w_gate.shape[1]
        turned_cache = [c.transpose(0, 2, 3, 1).reshape(rows, width, cache) for c in (k_cache, v_cache)]
        trig = jnp.asarray(rotary_table(heads, HEAD, cache - 1))
        half, groups, nf, nd = d // 2, rows // GROUP, ff // FCHUNK, d // DCHUNK
        dma = pltpu.SemaphoreType.DMA
        return pl.pallas_call(
            layer_kernel,
            out_shape=pltpu.VMEM((rows, d), BF16),
            in_specs=[pl.BlockSpec(memory_space=pl.ANY)] * 11,
            out_specs=pl.BlockSpec(memory_space=pltpu.VMEM),
            scratch_shapes=[
                pltpu.VMEM((SLOTS, width, cache), BF16),
                pltpu.VMEM((SLOTS, width, cache), BF16),
                pltpu.VMEM((d, ff), BF16),
                pltpu.VMEM((d, ff), BF16),
                pltpu.VMEM((ff, d), BF16),
                pltpu.VMEM((width, d), BF16),
                pltpu.VMEM((rows, d), BF16),
                pltpu.VMEM((d,), BF16),
                pltpu.VMEM((d,), BF16),
                pltpu.VMEM((3, width), F32),
                pltpu.VMEM((rows, width), F32),
                pltpu.VMEM((rows, width), F32),
                pltpu.VMEM((rows, half), F32),
                pltpu.VMEM((rows, half), BF16),
                pltpu.VMEM((rows, half), BF16),
                pltpu.VMEM((rows, half), BF16),
                pltpu.VMEM((rows, half), BF16),
                pltpu.VMEM((rows, d), BF16),
                pltpu.VMEM((rows, ff), BF16),
                pltpu.VMEM((rows, half), BF16),
                pltpu.VMEM((rows, half), BF16),
                pltpu.VMEM((rows, half), BF16),
                pltpu.VMEM((rows, half), BF16),
                pltpu.VMEM((PADDED, d), BF16),
                pltpu.VMEM((rows, DCHUNK), F32),
                dma((SLOTS,)), dma((SLOTS,)), dma((d // QCHUNK,)), dma, dma((ff // FSTEP,)), dma((ff // FSTEP,)), dma((nd,)), dma((4,)),
                dma, dma((groups,)), dma, dma((groups,)), dma, dma,
                dma, dma((nd,)), dma, dma((nd,)), dma, dma,
            ],
            compiler_params=pltpu.CompilerParams(
                collective_id=0, has_side_effects=True, vmem_limit_bytes=VMEM_LIMIT
            ),
            name="decode_layer",
        )(x, *turned_cache, gain_a, wq, wo, gain_m, w_gate, w_up, w_down, trig)

    states, cache, columns, rows_of = P("dp", None), P("dp", None, "tp", None), P(None, "tp"), P("tp", None)
    return jax.shard_map(
        step,
        mesh=mesh,
        in_specs=(states, cache, cache, P(None), columns, rows_of, P(None), columns, columns, rows_of),
        out_specs=states,
        check_vma=False,
    )
```

```python
import jax
import jax.numpy as jnp
import numpy as np
from jax import lax
from jax.experimental import pallas as pl
from jax.experimental.pallas import tpu as pltpu
from jax.sharding import PartitionSpec as P

HEAD = 96
THETA = 10000
EPS = 1e-6
VMEM_LIMIT = 66_500_000
EARLY = 3
SLOTS = 5
GROUP = 16
LAST = 4
QCHUNK = 1536
FCHUNK = 512
FSTEPS = (1024, 512, 512)
PADDED = 128
DCOPY = 1024
DCHUNK = 512
LAG = 1

F32, BF16 = jnp.float32, jnp.bfloat16
NT = (((1,), (1,)), ((), ()))


def rotary_table(heads, head, place):
    half = head // 2
    angle = np.float32(place) * np.float32(THETA) ** (-np.arange(half, dtype=np.float32) / np.float32(half))
    cos, sin, zero = np.cos(angle), np.sin(angle), np.zeros(half, np.float32)
    rows = [np.concatenate(r) for r in ((cos, cos), (-sin, zero), (zero, sin))]
    return np.stack([np.tile(r, heads) for r in rows]).astype(np.float32)


def dot(a, b):
    return jnp.dot(a, b, preferred_element_type=F32)


def normed(wide, gain):
    scale = lax.rsqrt(jnp.mean(wide * wide, -1, keepdims=True) + EPS)
    return (wide * scale * gain).astype(BF16)


def layer_kernel(
    x_hbm, k_hbm, v_hbm, ga_hbm, wq_hbm, wo_hbm, gm_hbm, wg_hbm, wu_hbm, wd_hbm, trig_hbm,
    y_ref,
    k_buf, v_buf, wg, wu, wd, wo, x, ga, gm, trig,
    q, o, term, send1, recv1, send2, recv2, h, hid,
    send3, recv3, send4, recv4, states, piece, last_send, last_recv,
    psem, qsem, wsem, fsem, dsem, isem,
    sa, sb, ls, lr, r2, r3, r4, r5,
):
    rows, d = x.shape
    width = q.shape[1]
    ff = hid.shape[1]
    half = d // 2
    heads = width // HEAD
    t = lax.axis_index("tp")
    core = lax.rem(t, 2)
    other = 1 - core
    partner = t + 1 - 2 * core
    across = lax.rem(t + 2, 4)
    diagonal = lax.rem(partner + 2, 4)
    groups = rows // GROUP
    nq, nf, nd = d // QCHUNK, ff // FCHUNK, d // DCHUNK
    dh = DCHUNK // 2

    barrier = pltpu.get_barrier_semaphore()
    for peer in (partner, across, diagonal):
        pl.semaphore_signal(barrier, inc=1, device_id={"tp": peer}, device_id_type=pl.DeviceIdType.MESH)

    def key_copy(i, sem):
        slot = lax.rem(i, SLOTS)
        return pltpu.make_async_copy(k_hbm.at[i], k_buf.at[slot], sem)

    def value_copy(i):
        slot = lax.rem(i, SLOTS)
        return pltpu.make_async_copy(v_hbm.at[i], v_buf.at[slot], psem.at[slot])

    def next_key_copy(i):
        return key_copy(i + 1, psem.at[lax.rem(i, SLOTS)])

    def wait_pair(i):
        two = pl.ds(0, 2)
        pltpu.make_async_copy(k_hbm.at[two], k_buf.at[two], psem.at[lax.rem(i, SLOTS)]).wait()

    wq = wg.at[:, pl.ds(0, width)]
    first = [
        pltpu.make_async_copy(x_hbm, x, isem.at[0]),
        pltpu.make_async_copy(ga_hbm, ga, isem.at[1]),
        pltpu.make_async_copy(trig_hbm, trig, isem.at[2]),
    ]
    query_copy = [
        pltpu.make_async_copy(wq_hbm.at[pl.ds(c * QCHUNK, QCHUNK)], wq.at[pl.ds(c * QCHUNK, QCHUNK)], qsem.at[c])
        for c in range(nq)
    ]
    later = [
        pltpu.make_async_copy(gm_hbm, gm, isem.at[3]),
        pltpu.make_async_copy(wo_hbm, wo, wsem),
    ]

    step_of = [k for k, size in enumerate(FSTEPS) for _ in range(size // FCHUNK)]

    def hidden_units(n):
        return pl.ds(pl.multiple_of(n * FCHUNK, FCHUNK), FCHUNK)

    def out_columns(n, size):
        return pl.ds(pl.multiple_of(n * size, size), size)

    def gate_copy(n):
        return pltpu.make_async_copy(wg_hbm.at[:, hidden_units(n)], wg.at[:, hidden_units(n)], fsem.at[step_of[n]])

    def up_copy(n):
        return pltpu.make_async_copy(wu_hbm.at[:, hidden_units(n)], wu.at[:, hidden_units(n)], fsem.at[step_of[n]])

    def weight_copy(n):
        return (up_copy if n % 2 else gate_copy)(n // 2)

    def down_copy(n):
        return pltpu.make_async_copy(wd_hbm.at[:, out_columns(n, DCOPY)], wd.at[:, out_columns(n, DCOPY)], dsem.at[n])

    for c in first + query_copy:
        c.start()
    first_keys = key_copy(0, isem.at[4])
    first_keys.start()
    for i in range(2):
        value_copy(i).start()
        next_key_copy(i).start()

    for c in first[:3]:
        c.wait()
    with jax.named_scope('norm_a'):
        a = normed(x[...].astype(F32), ga[...].astype(F32).reshape(1, d))
        states[0:rows, :] = a
        states[rows:PADDED, :] = jnp.zeros((PADDED - rows, d), BF16)
    for i in range(2, SLOTS - 1):
        value_copy(i).start()
        next_key_copy(i).start()
    for n in range(nq):
        with jax.named_scope('wait_wq'):
            query_copy[n].wait()
        part_q = dot(states[0:rows, n * QCHUNK:(n + 1) * QCHUNK], wg[n * QCHUNK:(n + 1) * QCHUNK, 0:width])
        if n == 0:
            q[...] = part_q
        else:
            q[...] += part_q
    value_copy(SLOTS - 1).start()
    for c in later:
        c.start()
    q0 = q[...].astype(BF16).astype(F32)
    ahead = pltpu.roll(q0, width - HEAD // 2, 1)
    behind = pltpu.roll(q0, HEAD // 2, 1)
    q[...] = (q0 * trig[0:1, :] + ahead * trig[1:2, :] + behind * trig[2:3, :]).astype(BF16).astype(F32)

    lane = lax.broadcasted_iota(jnp.int32, (heads, width), 1)
    top = lax.broadcasted_iota(jnp.int32, (heads, width), 0) * HEAD
    own_head = (lane >= top) & (lane < top + HEAD)

    o[...] = jnp.zeros_like(o)
    pl.semaphore_wait(barrier, 3)

    def to(peer, src, dst, ssem, rsem):
        return pltpu.make_async_remote_copy(
            src_ref=src, dst_ref=dst, send_sem=ssem, recv_sem=rsem,
            device_id={"tp": peer}, device_id_type=pl.DeviceIdType.MESH,
        )

    def sent(sem):
        three = pl.ds(0, 3 * rows // 2)
        return to(partner, wo.at[three], wo.at[three], sem, r3)

    mine = pl.ds(pl.multiple_of(core * half, half), half)
    theirs = pl.ds(pl.multiple_of(other * half, half), half)

    def rows_of(g):
        return pl.ds(pl.multiple_of(g * GROUP, GROUP), GROUP)

    def copy1(g):
        return to(partner, send1.at[rows_of(g)], recv1.at[rows_of(g)], sa, r4.at[g])

    def copy2(g):
        return to(across, send2.at[rows_of(g)], recv2.at[rows_of(g)], sa, r2.at[g])

    def copy3(g):
        return to(partner, h.at[rows_of(g), mine], h.at[rows_of(g), mine], sa, r3)

    def project(g):
        at = rows_of(g)
        seen = o[at, :].astype(BF16)
        send1[at, :] = dot(seen, wo[:, theirs]).astype(BF16)
        copy1(g).start()
        term[at, :] = dot(seen, wo[:, mine])

    def pair_sum(g):
        at = rows_of(g)
        copy1(g).wait_recv()
        send2[at, :] = (term[at, :] + recv1[at, :].astype(F32)).astype(BF16)
        copy2(g).start()

    def finish(g):
        at = rows_of(g)
        copy2(g).wait_recv()
        total = send2[at, :].astype(F32) + recv2[at, :].astype(F32)
        h[at, mine] = (x[at, mine].astype(F32) + total).astype(BF16)
        copy3(g).start()

    def softmax(scores):
        scores = scores * HEAD**-0.5
        e = jnp.exp(scores - jnp.max(scores, -1, keepdims=True))
        return (e / jnp.sum(e, -1, keepdims=True)).astype(BF16)

    def scores_of(i):
        row = q[pl.ds(i, 1), :]
        spread = jnp.where(own_head, jnp.broadcast_to(row, (heads, width)), 0.0).astype(BF16)
        return dot(spread, k_buf[lax.rem(i, SLOTS)])

    def add_values(i, weights):
        out = lax.dot_general(weights, v_buf[lax.rem(i, SLOTS)], NT, preferred_element_type=F32)
        o[pl.ds(i, 1), :] = jnp.sum(jnp.where(own_head, out, 0.0), 0, keepdims=True)

    first_keys.wait()
    weights = softmax(scores_of(0))
    next_key_copy(SLOTS - 1).start()

    def sequence(i, weights):
        with jax.named_scope('wait_cache'):
            wait_pair(i)
        scores = scores_of(i + 1)
        add_values(i, weights)
        weights = softmax(scores)

        @pl.when(i + 1 + SLOTS < rows)
        def _():
            next_key_copy(i + SLOTS).start()

        @pl.when(i + SLOTS < rows)
        def _():
            value_copy(i + SLOTS).start()

        for n in range(EARLY):
            @pl.when(i == rows - 1 - EARLY + n)
            def _():
                weight_copy(n).start()

        g = lax.div(i, GROUP)
        step = lax.rem(i, GROUP)

        @pl.when(i == GROUP - 1)
        def _():
            later[1].wait()

        @pl.when((step == GROUP - 1) | (i == rows - LAST - 1))
        def _():
            with jax.named_scope('project'):
                project(g)

        @pl.when((step == 1) & (i > GROUP))
        def _():
            with jax.named_scope('pair_sum'):
                pair_sum(g - 1)

        @pl.when(i == rows - LAST + 1)
        def _():
            with jax.named_scope('pair_sum'):
                pair_sum(groups - 1)

        @pl.when((step == 8) & (i > GROUP))
        def _():
            with jax.named_scope('finish'):
                finish(g - 1)

        return weights

    weights = lax.fori_loop(0, rows - 1, sequence, weights)
    for n in range(EARLY, 2 * nf):
        weight_copy(n).start()
    with jax.named_scope('last_cache'):
        value_copy(rows - 1).wait()
    add_values(rows - 1, weights)
    tail, block = pl.ds(rows - GROUP, GROUP), half // 4
    upper = lax.broadcasted_iota(jnp.int32, (8, block), 0) < LAST

    def last_copy(j, slot, peer):
        return to(peer, last_send.at[j], last_recv.at[slot, j], ls, lr)

    for j in range(2):
        with jax.named_scope('project_last'):
            seen = o[pl.ds(rows - 8, 8), :].astype(BF16)
            last_term = dot(seen, wo[:, j * half:(j + 1) * half])
            blocks = [last_term[:, k * block:(k + 1) * block] for k in range(4)]
            packed = [jnp.where(upper, pltpu.roll(blocks[k], LAST, 0), blocks[k + 1]) for k in (0, 2)]
            last_send[j] = jnp.concatenate(packed, 0).astype(BF16)
            for slot, peer in ((1, across), (2, diagonal), (0, partner)):
                last_copy(j, slot, peer).start()
    with jax.named_scope('finish'):
        finish(groups - 1)
    with jax.named_scope('wait_h'):
        to(partner, h.at[:, mine], h.at[:, mine], sa, r3).wait_recv()
        sent(sa).wait_send()
    later[0].wait()
    with jax.named_scope('wait_last'):
        to(partner, last_recv, last_recv, ls, lr).wait_recv()
    blocks = []
    for j in range(2):
        near = last_send[j].astype(F32) + last_recv[0, j].astype(F32)
        total = near + (last_recv[1, j].astype(F32) + last_recv[2, j].astype(F32))
        for packed in (total[:8], total[8:]):
            blocks += [pltpu.roll(packed, LAST, 0), packed]
    last_h = x[tail, :].astype(F32)[8:] + jnp.concatenate(blocks, 1)
    old = h[tail, :].astype(F32)
    keep = lax.broadcasted_iota(jnp.int32, (8, d), 0) < 8 - LAST
    h[tail, :] = jnp.concatenate([old[:8], jnp.where(keep, old[8:], last_h)], 0).astype(BF16)
    for n in range(d // DCOPY):
        down_copy(n).start()
    with jax.named_scope('norm_m'):
        states[0:rows, :] = normed(h[...].astype(F32), gm[...].astype(F32).reshape(1, d))

    done = 0
    for k, size in enumerate(FSTEPS):
        at, both = pl.ds(done, size), pl.ds(0, 2 * size)
        with jax.named_scope('wait_gate_up'):
            pltpu.make_async_copy(wg_hbm.at[:, both], wg.at[:, both], fsem.at[k]).wait()
        done += size
        gate = dot(states[...], wg[:, at])[:rows]
        up = dot(states[...], wu[:, at])[:rows]
        hid[:, at] = (gate * jax.nn.sigmoid(gate) * up).astype(BF16)

    def columns(n, which):
        return pl.ds(pl.multiple_of(n * DCHUNK + which * dh, dh), dh)

    def part(n):
        return pl.ds(pl.multiple_of(n * dh, dh), dh)

    def copy4(n):
        return to(partner, send3.at[:, part(n)], recv3.at[:, part(n)], sb, r4.at[n])

    def copy5(n):
        return to(across, send4.at[:, part(n)], recv4.at[:, part(n)], sb, r5.at[n])

    def copy6(n):
        return to(partner, y_ref.at[:, columns(n, core)], y_ref.at[:, columns(n, core)], sb, r3)

    def down(n):
        @pl.when(lax.rem(n, DCOPY // DCHUNK) == 0)
        def _():
            with jax.named_scope('wait_down'):
                down_copy(lax.div(n, DCOPY // DCHUNK)).wait()

        piece[...] = dot(hid[...], wd[:, out_columns(n, DCHUNK)])
        send3[:, part(n)] = piece[:, pl.ds(pl.multiple_of(other * dh, dh), dh)].astype(BF16)
        copy4(n).start()
        term[:, part(n)] = piece[:, pl.ds(pl.multiple_of(core * dh, dh), dh)]

    def down_pair(n):
        with jax.named_scope('wait_pair'):
            copy4(n).wait_recv()
        send4[:, part(n)] = (term[:, part(n)] + recv3[:, part(n)].astype(F32)).astype(BF16)
        copy5(n).start()

    def down_finish(n, carry):
        with jax.named_scope('wait_across'):
            copy5(n).wait_recv()
        total = send4[:, part(n)].astype(F32) + recv4[:, part(n)].astype(F32)
        y_ref[:, columns(n, core)] = (h[:, columns(n, core)].astype(F32) + total).astype(BF16)
        copy6(n).start()
        return carry

    def down_step(n, carry):
        @pl.when(n < nd)
        def _():
            down(n)

        @pl.when(n >= LAG)
        def _():
            down_pair(n - LAG)

        return carry

    lax.fori_loop(0, nd + LAG, down_step, 0)
    lax.fori_loop(0, nd, down_finish, 0)
    with jax.named_scope('wait_y'):
        to(partner, y_ref.at[:, mine], y_ref.at[:, mine], sb, r3).wait_recv()
    with jax.named_scope('send_waits'):
        sent(sb).wait_send()
        to(partner, last_recv, last_recv, ls, lr).wait_send()


def solution(mesh):
    def step(x, k_cache, v_cache, gain_a, wq, wo, gain_m, w_gate, w_up, w_down):
        rows, d = x.shape
        cache, heads = k_cache.shape[1:3]
        width = heads * HEAD
        ff = w_gate.shape[1]
        turned_cache = [c.transpose(0, 2, 3, 1).reshape(rows, width, cache) for c in (k_cache, v_cache)]
        trig = jnp.asarray(rotary_table(heads, HEAD, cache - 1))
        half, groups, nf, nd = d // 2, rows // GROUP, ff // FCHUNK, d // DCHUNK
        dma = pltpu.SemaphoreType.DMA
        return pl.pallas_call(
            layer_kernel,
            out_shape=pltpu.VMEM((rows, d), BF16),
            in_specs=[pl.BlockSpec(memory_space=pl.ANY)] * 11,
            out_specs=pl.BlockSpec(memory_space=pltpu.VMEM),
            scratch_shapes=[
                pltpu.VMEM((SLOTS, width, cache), BF16),
                pltpu.VMEM((SLOTS, width, cache), BF16),
                pltpu.VMEM((d, ff), BF16),
                pltpu.VMEM((d, ff), BF16),
                pltpu.VMEM((ff, d), BF16),
                pltpu.VMEM((width, d), BF16),
                pltpu.VMEM((rows, d), BF16),
                pltpu.VMEM((d,), BF16),
                pltpu.VMEM((d,), BF16),
                pltpu.VMEM((3, width), F32),
                pltpu.VMEM((rows, width), F32),
                pltpu.VMEM((rows, width), F32),
                pltpu.VMEM((rows, half), F32),
                pltpu.VMEM((rows, half), BF16),
                pltpu.VMEM((rows, half), BF16),
                pltpu.VMEM((rows, half), BF16),
                pltpu.VMEM((rows, half), BF16),
                pltpu.VMEM((rows, d), BF16),
                pltpu.VMEM((rows, ff), BF16),
                pltpu.VMEM((rows, half), BF16),
                pltpu.VMEM((rows, half), BF16),
                pltpu.VMEM((rows, half), BF16),
                pltpu.VMEM((rows, half), BF16),
                pltpu.VMEM((PADDED, d), BF16),
                pltpu.VMEM((rows, DCHUNK), F32),
                pltpu.VMEM((2, GROUP, d // 8), BF16),
                pltpu.VMEM((3, 2, GROUP, d // 8), BF16),
                dma((SLOTS,)), dma((d // QCHUNK,)), dma, dma((len(FSTEPS),)), dma((d // DCOPY,)), dma((5,)),
                dma, dma, dma, dma, dma((groups,)), dma, dma((nd,)), dma((nd,)),
            ],
            compiler_params=pltpu.CompilerParams(
                collective_id=0, has_side_effects=True, vmem_limit_bytes=VMEM_LIMIT
            ),
            name="decode_layer",
        )(x, *turned_cache, gain_a, wq, wo, gain_m, w_gate, w_up, w_down, trig)

    states, cache, columns, rows_of = P("dp", None), P("dp", None, "tp", None), P(None, "tp"), P("tp", None)
    return jax.shard_map(
        step,
        mesh=mesh,
        in_specs=(states, cache, cache, P(None), columns, rows_of, P(None), columns, columns, rows_of),
        out_specs=states,
        check_vma=False,
    )
```
